32 devices in a mesh: stream: 4 (over x, core), cross: 8 (over z, y).
Axes of the slice: x: 2, y: 2, z: 4, core: 2. Of those that a mesh axis runs over, the one named last changes fastest.
Arguments:
- state_now: float32 [7, 8, 64, 512], P(None, None, 'cross', 'stream'), as said below
- state_base: float32 [7, 8, 64, 512], P(None, None, 'cross', 'stream'), as said below
- inflow: float32 [7, 8, 64, 3], P(None, None, 'cross'), as said below
Outputs:
- state_next: float32 [7, 8, 64, 512], P(None, None, 'cross', 'stream')
Inputs may be any that keep to these rules, and one draw needn't show every extreme that they name: `state_now`: partial densities and volume fractions are positive, volume fractions below 1, and the pressure that each cell implies is positive. `state_base`: partial densities and volume fractions are positive, volume fractions below 1, and the pressure that each cell implies is positive. `inflow`: partial densities and volume fractions are positive, volume fractions below 1, and the pressure that each cell implies is positive.
All inputs are finite; a program needn't handle non-finite values.
Results may differ from the reference program's by a relative error of at most 0.0003.
Values sent between devices are 32-bit elements; how exact they have to be, the bound alone decides.
A program may use at most 64 MiB of HBM per device.

```python
import jax
import jax.numpy as jnp
from jax import lax

CZ = 8
NX = 512
NY = 64


gas_gamma = 1.4


liquid_gamma = 4.4


liquid_stiff = 0.6


def field_cells(key, streamwise):
    subkeys = jax.random.split(key, 7)
    grid_shape = streamwise.shape
    lower_end = 0.5
    upper_end = 2.0
    volume = jax.random.uniform(subkeys[2], grid_shape, jnp.float32, 0.1, 0.9)

    def rough_field(subkey):
        return jnp.exp(jax.random.uniform(subkey, grid_shape, jnp.float32, jnp.log(lower_end), jnp.log(upper_end)))
    dens_gas = rough_field(subkeys[0])
    dens_liquid = 4.0 * rough_field(subkeys[1])
    stream_vel = (0.4 + 6.0 * streamwise) * jax.random.uniform(subkeys[3], grid_shape, jnp.float32, 0.8, 1.2)
    cross_vel = jax.random.uniform(subkeys[4], grid_shape, jnp.float32, -0.8, 0.8)
    span_vel = jax.random.uniform(subkeys[5], grid_shape, jnp.float32, -0.8, 0.8)
    pressure = rough_field(subkeys[6])
    partial_gas = volume * dens_gas
    partial_liquid = (1.0 - volume) * dens_liquid
    density = partial_gas + partial_liquid
    stiff_gamma = volume / (gas_gamma - 1.0) + (1.0 - volume) / (liquid_gamma - 1.0)
    stiff_term = (1.0 - volume) * liquid_gamma * liquid_stiff / (liquid_gamma - 1.0)
    energy = stiff_gamma * pressure + stiff_term + 0.5 * density * (stream_vel * stream_vel + cross_vel * cross_vel + span_vel * span_vel)
    return jnp.stack([partial_gas, partial_liquid, density * stream_vel, density * cross_vel, density * span_vel, energy, volume])


def grid_positions():
    positions = (jnp.arange(NX, dtype=jnp.float32) + 0.5) / NX
    return jnp.broadcast_to(positions, (CZ, NY, NX))


def draw_state_now(key, part):
    return field_cells(jax.random.fold_in(key, 11), grid_positions())


def draw_state_base(key, part):
    return field_cells(jax.random.fold_in(key, 23), grid_positions())


def draw_inflow(key, part):
    return field_cells(jax.random.fold_in(key, 37), jnp.ones((CZ, NY, 3), jnp.float32))


def setup_inputs(seed: int = 0) -> dict:
    key_list = jax.random.split(jax.random.key(seed), 4)
    return {
        "state_now": draw_state_now(jax.random.fold_in(key_list[3], 71), 0),
        "state_base": draw_state_base(jax.random.fold_in(key_list[3], 71), 0),
        "inflow": draw_inflow(jax.random.fold_in(key_list[3], 71), 0),
    }


gas_gamma = 1.4
liquid_gamma = 4.4
liquid_stiff = 0.6
courant = 0.3
weno_epsilon = 1e-06

def mixture(volume):
    stiff_gamma = volume / (gas_gamma - 1.0) + (1.0 - volume) / (liquid_gamma - 1.0)
    stiff_term = (1.0 - volume) * liquid_gamma * liquid_stiff / (liquid_gamma - 1.0)
    return (stiff_gamma, stiff_term)

def primitive(conserved):
    density = conserved[0] + conserved[1]
    vel_one = conserved[2] / density
    vel_two = conserved[3] / density
    vel_three = conserved[4] / density
    kinetic = 0.5 * (conserved[2] * vel_one + conserved[3] * vel_two + conserved[4] * vel_three)
    stiff_gamma, stiff_term = mixture(conserved[6])
    pressure = (conserved[5] - kinetic - stiff_term) / stiff_gamma
    return jnp.stack([conserved[0], conserved[1], vel_one, vel_two, vel_three, pressure, conserved[6]])

def sound(primitives):
    density = primitives[0] + primitives[1]
    stiff_gamma, stiff_term = mixture(primitives[6])
    return jnp.sqrt(((stiff_gamma + 1.0) * primitives[5] + stiff_term) / (stiff_gamma * density))

def max_speed(conserved):
    primitives = primitive(conserved)
    fastest = jnp.maximum(jnp.maximum(jnp.abs(primitives[2]), jnp.abs(primitives[3])), jnp.abs(primitives[4]))
    return jnp.max(fastest + sound(primitives))

def weno_face(far_left, near_left, centre, near_right, far_right):
    first_low = far_left - 2.0 * near_left + centre
    second_low = far_left - 4.0 * near_left + 3.0 * centre
    first_mid = near_left - 2.0 * centre + near_right
    second_mid = near_left - near_right
    first_high = centre - 2.0 * near_right + far_right
    second_high = 3.0 * centre - 4.0 * near_right + far_right
    smooth_low = weno_epsilon + 13.0 / 12.0 * first_low * first_low + 0.25 * second_low * second_low
    smooth_mid = weno_epsilon + 13.0 / 12.0 * first_mid * first_mid + 0.25 * second_mid * second_mid
    smooth_high = weno_epsilon + 13.0 / 12.0 * first_high * first_high + 0.25 * second_high * second_high
    weight_low = 0.1 / (smooth_low * smooth_low)
    weight_mid = 0.6 / (smooth_mid * smooth_mid)
    weight_high = 0.3 / (smooth_high * smooth_high)
    guess_low = (2.0 * far_left - 7.0 * near_left + 11.0 * centre) / 6.0
    guess_mid = (-near_left + 5.0 * centre + 2.0 * near_right) / 6.0
    guess_high = (2.0 * centre + 5.0 * near_right - far_right) / 6.0
    return (weight_low * guess_low + weight_mid * guess_mid + weight_high * guess_high) / (weight_low + weight_mid + weight_high)

def clamp_face(state, lower_cell, upper_cell):
    smaller = jnp.minimum(lower_cell, upper_cell)
    larger = jnp.maximum(lower_cell, upper_cell)
    limited = []
    for component in range(7):
        face_value = state[component]
        if component in (0, 1, 5):
            face_value = jnp.maximum(face_value, 0.5 * smaller[component])
        elif component == 6:
            face_value = jnp.clip(face_value, 0.5 * smaller[6], 1.0 - 0.5 * (1.0 - larger[6]))
        limited.append(face_value)
    return jnp.stack(limited)

def side_terms(primitives, normal):
    density = primitives[0] + primitives[1]
    stiff_gamma, stiff_term = mixture(primitives[6])
    velocity = [primitives[2], primitives[3], primitives[4]]
    energy = stiff_gamma * primitives[5] + stiff_term + 0.5 * density * (velocity[0] * velocity[0] + velocity[1] * velocity[1] + velocity[2] * velocity[2])
    normal_vel = velocity[normal]
    amounts = jnp.stack([primitives[0], primitives[1], density * velocity[0], density * velocity[1], density * velocity[2], energy, primitives[6]])
    momentum = []
    for component in range(3):
        moved = density * velocity[component] * normal_vel
        if component == normal:
            moved = moved + primitives[5]
        momentum.append(moved)
    transport = jnp.stack([primitives[0] * normal_vel, primitives[1] * normal_vel, momentum[0], momentum[1], momentum[2], (energy + primitives[5]) * normal_vel, primitives[6] * normal_vel])
    signal = jnp.abs(normal_vel) + sound(primitives)
    return (amounts, transport, normal_vel, signal)

def face_flux(left_state, right_state, normal):
    amount_left, transport_left, normal_left, signal_left = side_terms(left_state, normal)
    amount_right, transport_right, normal_right, signal_right = side_terms(right_state, normal)
    fastest = jnp.maximum(signal_left, signal_right)
    face_fluxes = 0.5 * (transport_left + transport_right) - 0.5 * fastest * (amount_right - amount_left)
    return (face_fluxes, 0.5 * (normal_left + normal_right))

def direction_sweep(padded, dimension, normal):
    primitives = primitive(padded)
    length = padded.shape[dimension] - 6
    pieces = [lax.slice_in_dim(primitives, offset, offset + length + 1, axis=dimension) for offset in range(6)]
    left_state = clamp_face(weno_face(pieces[0], pieces[1], pieces[2], pieces[3], pieces[4]), pieces[2], pieces[3])
    right_state = clamp_face(weno_face(pieces[5], pieces[4], pieces[3], pieces[2], pieces[1]), pieces[2], pieces[3])
    face_fluxes, face_motion = face_flux(left_state, right_state, normal)
    change = lax.slice_in_dim(face_fluxes, 1, length + 1, axis=dimension) - lax.slice_in_dim(face_fluxes, 0, length, axis=dimension)
    spread = lax.slice_in_dim(face_motion, 1, length + 1, axis=dimension - 1) - lax.slice_in_dim(face_motion, 0, length, axis=dimension - 1)
    return (change, spread)

def tendency(stream_cells, cross_cells, span_cells, centre_cells):
    change_stream, spread_stream = direction_sweep(stream_cells, 3, 0)
    change_cross, spread_cross = direction_sweep(cross_cells, 2, 1)
    change_span, spread_span = direction_sweep(span_cells, 1, 2)
    total = -(change_stream + change_cross + change_span)
    source = centre_cells[6] * (spread_stream + spread_cross + spread_span)
    return jnp.concatenate([total[:6], (total[6] + source)[None]], axis=0)

def reference(state_now, state_base, inflow):

    def plane_max(plane_index):
        return max_speed(lax.dynamic_slice_in_dim(state_base, plane_index, 1, 1))
    fastest = jnp.max(lax.map(plane_max, jnp.arange(CZ, dtype=jnp.int32)))
    time_step = courant / fastest
    last_cells = jnp.repeat(state_now[:, :, :, -1:], 3, axis=3)
    stream_padded = jnp.concatenate([inflow, state_now, last_cells], axis=3)
    cross_padded = jnp.concatenate([stream_padded[:, :, -3:], stream_padded, stream_padded[:, :, :3]], axis=2)
    padded = jnp.concatenate([cross_padded[:, -3:], cross_padded, cross_padded[:, :3]], axis=1)

    def one_plane(plane_index):
        span_cells = lax.dynamic_slice_in_dim(padded, plane_index, 7, 1)[:, :, 3:-3, 3:-3]
        middle = lax.dynamic_slice_in_dim(padded, plane_index + 3, 1, 1)
        cross_cells = middle[:, :, :, 3:-3]
        stream_cells = middle[:, :, 3:-3, :]
        centre_cells = middle[:, :, 3:-3, 3:-3]
        changes = tendency(stream_cells, cross_cells, span_cells, centre_cells)
        base_plane = lax.dynamic_slice_in_dim(state_base, plane_index, 1, 1)
        updated = base_plane / 3.0 + 2.0 / 3.0 * (centre_cells + time_step * changes)
        return updated[:, 0]
    planes = lax.map(one_plane, jnp.arange(CZ, dtype=jnp.int32))
    return jnp.transpose(planes, (1, 0, 2, 3))
```

```python
import functools

import jax
import jax.numpy as jnp
from jax import lax
from jax.experimental import pallas as pl
from jax.experimental.pallas import tpu as pltpu
from jax.sharding import PartitionSpec as P

MESH = pl.DeviceIdType.MESH
VARS = 7
HALO = 3
GROUP = 8
DIRECT = 64
HUBS = 2
STIFF = 4.4 * 0.6 / 3.4


def recip(x):
    return 1.0 / x


def mixture(volume):
    rest = 1.0 - volume
    return volume * (1.0 / 0.4) + rest * (1.0 / 3.4), rest * STIFF


def primitive(u):
    inv = recip(u[0] + u[1])
    vx, vy, vz = u[2] * inv, u[3] * inv, u[4] * inv
    gam, stiff = mixture(u[6])
    kinetic = 0.5 * (u[2] * vx + u[3] * vy + u[4] * vz)
    return [u[0], u[1], vx, vy, vz, (u[5] - kinetic - stiff) * recip(gam), u[6]]


def max_speed(w):
    gam, stiff = mixture(w[6])
    top = (gam + 1.0) * w[5] + stiff
    sound = jnp.sqrt(top * recip(gam * (w[0] + w[1])))
    return jnp.maximum(jnp.maximum(jnp.abs(w[2]), jnp.abs(w[3])), jnp.abs(w[4])) + sound


def weno_pair(f, g, h, k, l):
    e1, e2, e3, e4 = g - f, h - g, k - h, l - k
    s0, s1, s2 = e2 - e1, e3 - e2, e4 - e3
    d2, d3 = e2 + e2, e3 + e3
    t0, t1, t2 = d2 + s0, e2 + e3, d3 - s2
    eps = 1e-6 * 12.0 / 13.0
    r0 = recip(s0 * s0 + (eps + (3.0 / 13.0) * (t0 * t0)))
    r1 = recip(s1 * s1 + (eps + (3.0 / 13.0) * (t1 * t1)))
    r2 = recip(s2 * s2 + (eps + (3.0 / 13.0) * (t2 * t2)))
    a0, a1, a2 = r0 * r0, 6.0 * (r1 * r1), r2 * r2
    b0, b2 = 3.0 * a0, 3.0 * a2
    p0, p2 = t0 + e2, t2 + e3
    up = (a0 * (p0 + s0) + a1 * (d3 + e2) + b2 * p2) * recip(6.0 * (a0 + a1 + b2))
    down = (a2 * (p2 - s2) + a1 * (d2 + e3) + b0 * p0) * recip(6.0 * (a2 + a1 + b0))
    return h + up, h - down


def limit(state, low, high):
    out = list(state)
    for v in (0, 1, 5):
        out[v] = jnp.maximum(state[v], low[v])
    out[6] = jnp.minimum(jnp.maximum(state[6], low[6]), high)
    return out


def side(w, normal):
    dens = w[0] + w[1]
    gam, stiff = mixture(w[6])
    m = [dens * w[2], dens * w[3], dens * w[4]]
    heat = gam * w[5] + stiff
    energy = heat + 0.5 * (m[0] * w[2] + m[1] * w[3] + m[2] * w[4])
    vn = w[2 + normal]
    amounts = [w[0], w[1], m[0], m[1], m[2], energy, w[6]]
    moved = [q * vn for q in amounts]
    moved[2 + normal] = moved[2 + normal] + w[5]
    moved[5] = (energy + w[5]) * vn
    sound = jnp.sqrt((heat + w[5]) * recip(gam * dens))
    return amounts, moved, vn, jnp.abs(vn) + sound


def faces(left, right, below, above, normal):
    low = {v: 0.5 * jnp.minimum(below[v], above[v]) for v in (0, 1, 5, 6)}
    high = 1.0 - 0.5 * (1.0 - jnp.maximum(below[6], above[6]))
    ul, fl, nl, sl = side(limit(left, low, high), normal)
    ur, fr, nr, sr = side(limit(right, low, high), normal)
    fast = 0.5 * jnp.maximum(sl, sr)
    out = [0.5 * (fl[v] + fr[v]) - fast * (ur[v] - ul[v]) for v in range(VARS)]
    return out + [0.5 * (nl + nr)]


def rate(lo, hi, volume):
    out = [lo[v] - hi[v] for v in range(VARS)]
    out[6] = out[6] + volume * (hi[7] - lo[7])
    return out


def reader(src, height):
    def at(c, v):
        return src[pl.ds(pl.multiple_of((c * VARS + v) * height, height), height), :]

    def row(c):
        return [at(c, v) for v in range(VARS)]

    def states(c):
        pairs = [weno_pair(*[at(c + o, v) for o in range(-2, 3)]) for v in range(VARS)]
        return [p[0] for p in pairs], [p[1] for p in pairs]

    return at, row, states


def sweep(src, count, height, normal, emit):
    at, row, states = reader(src, height)

    def cell(c, left):
        after, right = states(c)
        return faces(left, right, row(c - 1), row(c), normal), after

    flux, left = cell(HALO, states(HALO - 1)[0])

    def step(i, carry):
        left, lo = carry
        hi, left = cell(i + HALO + 1, left)
        emit(i, rate(lo, hi, at(i + HALO, 6)))
        return left, hi

    lax.fori_loop(0, count, step, (left, flux))


def kernel(
    dims,
    direct,
    now_hbm,
    base_hbm,
    inflow_hbm,
    kept,
    total,
    scale,
    now,
    base,
    inflow,
    flat,
    wide,
    wz,
    wy,
    shifted,
    sided,
    fluxes,
    pack,
    from_low,
    from_high,
    joint,
    top_first,
    top_second,
    mine,
    load_sem,
    halo_send,
    halo_recv,
    first_send,
    first_recv,
    second_send,
    second_recv,
):
    n_stream, n_cross, cz, ny, nx = dims
    tile = VARS * ny
    ztile = VARS * cz
    half = cz * GROUP
    ms, mc = lax.axis_index("stream"), lax.axis_index("cross")

    loads = [
        pltpu.make_async_copy(base_hbm, base, load_sem.at[0]),
        pltpu.make_async_copy(now_hbm, now, load_sem.at[1]),
        pltpu.make_async_copy(inflow_hbm, inflow, load_sem.at[2]),
    ]
    for copy in loads:
        copy.start()

    size = n_stream * n_cross
    across = [(0, d) for d in range(1, n_cross)]
    along = [(d, 0) for d in range(1, n_stream)]
    others = [(d, e) for e in range(n_cross) for d in range(n_stream) if (d, e) != (0, 0)]
    inner, outer = ms > 0, ms < n_stream - 1
    hubs = [(ms == h) & (mc == 0) for h in range(HUBS)]
    early = functools.reduce(jnp.logical_or, hubs)
    caster = hubs[HUBS - 1]

    def device(offset):
        return {
            "stream": lax.rem(ms + offset[0], n_stream),
            "cross": lax.rem(mc + offset[1], n_cross),
        }

    barrier = pltpu.get_barrier_semaphore()

    def greet(target):
        pl.semaphore_signal(barrier, device_id=target, device_id_type=MESH)

    if direct:
        for h in range(HUBS):

            @pl.when(jnp.logical_not(hubs[h]))
            def _(h=h):
                greet({"stream": h, "cross": 0})

        for d in (1, n_cross - 1):
            greet(device((0, d)))
        pl.when(outer)(lambda: greet(device((1, 0))))
        pl.when(inner)(lambda: greet(device((n_stream - 1, 0))))

        @pl.when(early)
        def _():
            for p in others:
                greet(device(p))

        sides = jnp.where(inner, 1, 0) + jnp.where(outer, 1, 0)
        expected = 2 + sides + jnp.where(early, HUBS - 1 + size - 1, HUBS)
    else:
        for p in across + along:
            greet(device(p))
        expected = n_cross + n_stream - 2

    def remote(src, dst, send, recv, target):
        return pltpu.make_async_remote_copy(
            src_ref=src,
            dst_ref=dst,
            send_sem=send,
            recv_sem=recv,
            device_id=target,
            device_id_type=MESH,
        )

    def spread(slot, buffer, offsets, send, recv):
        return [
            remote(mine.at[slot], buffer.at[i], send, recv, device(p))
            for i, p in enumerate(offsets)
        ]

    def arrivals(buffer, count, recv):
        part = buffer.at[pl.ds(0, count)]
        pltpu.make_async_copy(part, part, recv).wait()

    first_out, first_in = first_send.at[0], first_recv.at[0]
    second_out, second_in = second_send.at[0], second_recv.at[0]
    if direct:
        spot_here = ms * n_cross + mc
        to_hub = [
            remote(
                mine.at[0],
                top_first.at[spot_here],
                first_send.at[h],
                first_in,
                {"stream": h, "cross": 0},
            )
            for h in range(HUBS)
        ]
        cast = [
            remote(mine.at[1], mine.at[2], second_out, second_in, {"stream": d, "cross": e})
            for e in range(n_cross)
            for d in range(n_stream)
            if e > 0 or d >= HUBS
        ]
    else:
        first = spread(0, top_first, across, first_out, first_in)
        second = spread(1, top_second, along, second_out, second_in)

    def greet_and_reduce():
        pl.semaphore_wait(barrier, expected)
        if direct:
            for h in range(HUBS):
                pl.when(jnp.logical_not(hubs[h]))(to_hub[h].start)
        else:
            for copy in first:
                copy.start()

    loads[0].wait()
    speed = None
    for z in range(cz):
        s = max_speed(primitive([base[v, z] for v in range(VARS)]))
        speed = s if speed is None else jnp.maximum(speed, s)
    mine[0] = jnp.max(speed, axis=0, keepdims=True)
    if direct:
        top_first[spot_here] = mine[0]

    if direct:
        pl.when(jnp.logical_not(early))(greet_and_reduce)
    else:
        greet_and_reduce()

    loads[1].wait()
    lane = lax.broadcasted_iota(jnp.int32, (ny, nx), 1)
    group = lane // GROUP
    packed = [None] * VARS
    for z in range(cz):
        w = primitive([now[v, z] for v in range(VARS)])
        spots = [HALO + z]
        if z < HALO:
            spots.append(HALO + cz + z)
        if z >= cz - HALO:
            spots.append(z - (cz - HALO))
        for v in range(VARS):
            for c in spots:
                wz[pl.ds(c * tile + v * ny, ny), :] = w[v]
            upper = pltpu.roll(w[v], (GROUP * z - (nx - 5)) % nx, 1)
            lower = pltpu.roll(w[v], (half + GROUP * z + HALO) % nx, 1)
            piece = jnp.where(group == z, upper, lower)
            if z == 0:
                packed[v] = piece
            else:
                packed[v] = jnp.where((group == z) | (group == cz + z), piece, packed[v])
    for v in range(VARS):
        pack[pl.ds(v * ny, ny), :] = packed[v]
    for y in range(ny):
        for v in range(VARS):
            wy[pl.ds((HALO + y) * ztile + v * cz, cz), :] = wz[
                pl.ds(HALO * tile + v * ny + y, cz, stride=tile), :
            ]

    rows = HALO * ztile
    halo_y = [
        pltpu.make_async_remote_copy(
            src_ref=wy.at[pl.ds(rows, rows)],
            dst_ref=wy.at[pl.ds((HALO + ny) * ztile, rows)],
            send_sem=halo_send.at[0],
            recv_sem=halo_recv.at[0],
            device_id=device((0, n_cross - 1)),
            device_id_type=MESH,
        ),
        pltpu.make_async_remote_copy(
            src_ref=wy.at[pl.ds(ny * ztile, rows)],
            dst_ref=wy.at[pl.ds(0, rows)],
            send_sem=halo_send.at[1],
            recv_sem=halo_recv.at[1],
            device_id=device((0, 1)),
            device_id_type=MESH,
        ),
    ]
    to_high = pltpu.make_async_remote_copy(
        src_ref=pack,
        dst_ref=from_low,
        send_sem=halo_send.at[2],
        recv_sem=halo_recv.at[2],
        device_id=device((1, 0)),
        device_id_type=MESH,
    )
    to_low = pltpu.make_async_remote_copy(
        src_ref=pack,
        dst_ref=from_high,
        send_sem=halo_send.at[3],
        recv_sem=halo_recv.at[3],
        device_id=device((n_stream - 1, 0)),
        device_id_type=MESH,
    )

    def send_up():
        halo_y[1].start()
        pl.when(outer)(to_high.start)
        pl.when(inner)(to_low.start)

    def send_down():
        halo_y[0].start()

    if direct:
        pl.when(jnp.logical_not(early))(send_up)
    else:
        send_up()

    def stream_shifts(w):
        return [[pltpu.roll(x, d % nx, 1) for x in w] for d in (2, 1, -1, -2)]

    def stream_states(shifts, w):
        m2, m1, p1, p2 = shifts
        pairs = [weno_pair(m2[v], m1[v], w[v], p1[v], p2[v]) for v in range(VARS)]
        return [pltpu.roll(p[0], 1, 1) for p in pairs], [p[1] for p in pairs]

    def ahead(lo):
        return [pltpu.roll(f, nx - 1, 1) for f in lo]

    def cell_rows(v, z):
        return pl.ds(pl.multiple_of((v * cz + z) * ny, ny), ny)

    def keep_rate(z, out):
        for v in range(VARS):
            total[cell_rows(v, z), :] = out[v]

    sweep(wz, cz, ny, 2, keep_rate)

    if direct:
        pl.when(jnp.logical_not(early))(send_down)
    else:
        send_down()

    whole = (lane >= HALO) & (lane < nx - 2)

    def centre(z):
        return [
            wz[pl.ds(pl.multiple_of(((HALO + z) * VARS + v) * ny, ny), ny), :]
            for v in range(VARS)
        ]

    def stage_shift(z):
        for d, row in enumerate(stream_shifts(centre(z))):
            for v in range(VARS):
                shifted[d, v] = row[v]

    def stage_state(z):
        shifts = [[shifted[d, v] for v in range(VARS)] for d in range(4)]
        left, right = stream_states(shifts, centre(z))
        for v in range(VARS):
            sided[0, v] = left[v]
            sided[1, v] = right[v]
            sided[2, v] = shifts[1][v]

    def stage_flux(z):
        left, right, below = [[sided[k, v] for v in range(VARS)] for k in range(3)]
        lo = [jnp.where(whole, f, 0.0) for f in faces(left, right, below, centre(z), 0)]
        hi = ahead(lo)
        for o in range(VARS + 1):
            fluxes[0, o] = lo[o]
            fluxes[1, o] = hi[o]

    def stage_rate(z):
        lo, hi = [[fluxes[k, o] for o in range(VARS + 1)] for k in range(2)]
        out = rate(lo, hi, centre(z)[6])
        for v in range(VARS):
            total[cell_rows(v, z), :] = total[cell_rows(v, z), :] + out[v]

    stages = (stage_shift, stage_state, stage_flux, stage_rate)
    depth = len(stages)

    def advance(z):
        for k in reversed(range(depth)):
            stages[k](z - k)

    for z in range(depth - 1):
        for k in reversed(range(z + 1)):
            stages[k](z - k)
    lax.fori_loop(depth - 1, cz, lambda z, c: (advance(z), c)[1], 0)
    for z in range(cz, cz + depth - 1):
        for k in reversed(range(z - cz + 1, depth)):
            stages[k](z - k)

    def add_rate(y, out):
        for v in range(VARS):
            rows = pl.ds(v * cz * ny + y, cz, stride=ny)
            total[rows, :] = total[rows, :] + out[v]

    wy_at, wy_row, wy_states = reader(wy, cz)

    def cross_face(y, left, right):
        return faces(left, right, wy_row(HALO + y - 1), wy_row(HALO + y), 1)

    def cross_rate(y, lo, hi):
        add_rate(y, rate(lo, hi, wy_at(HALO + y, 6)))

    def save(slot, values):
        for k, x in enumerate(values):
            joint[slot, k] = x

    def saved(slot, size):
        return [joint[slot, k] for k in range(size)]

    left, right = wy_states(2 * HALO - 1)
    save(0, right)
    lo = None
    for y in range(HALO, ny - HALO + 1):
        after, right = wy_states(HALO + y)
        hi = cross_face(y, left, right)
        if lo is None:
            save(1, hi)
        else:
            cross_rate(y - 1, lo, hi)
        left, lo = after, hi
    save(2, left)
    save(3, lo)

    def low_edge():
        left, _ = wy_states(HALO - 1)
        lo = None
        for y in range(HALO):
            if y < HALO - 1:
                after, right = wy_states(HALO + y)
            else:
                after, right = None, saved(0, VARS)
            hi = cross_face(y, left, right)
            if lo is not None:
                cross_rate(y - 1, lo, hi)
            left, lo = after, hi
        cross_rate(HALO - 1, lo, saved(1, VARS + 1))

    def high_edge():
        left, lo = saved(2, VARS), saved(3, VARS + 1)
        for y in range(ny - HALO + 1, ny + 1):
            after, right = wy_states(HALO + y)
            hi = cross_face(y, left, right)
            cross_rate(y - 1, lo, hi)
            left, lo = after, hi

    if direct:

        @pl.when(early)
        def _():
            greet_and_reduce()
            send_up()
            send_down()

    else:
        arrivals(top_first, len(across), first_in)
        slab = mine[0]
        for d in range(len(across)):
            slab = jnp.maximum(slab, top_first[d])
        mine[1] = slab
        for copy in second:
            copy.start()

    loads[2].wait()

    @pl.when(ms == 0)
    def _():
        for k in range(HALO):
            for v in range(VARS):
                flat[k, :, pl.ds(v * ny, ny)] = inflow[v, k]
            wide[pl.ds(half + k, cz, stride=GROUP), :] = flat[k]
        turned = jnp.transpose(wide[...])
        w = primitive([turned[v * ny : (v + 1) * ny] for v in range(VARS)])
        for v in range(VARS):
            from_low[pl.ds(v * ny, ny), :] = w[v]

    @pl.when(ms > 0)
    def _():
        to_high.wait_recv()

    spot = lane % GROUP

    @pl.when(ms == n_stream - 1)
    def _():
        for v in range(VARS):
            own = pack[pl.ds(v * ny, ny), :]
            copies = [pltpu.roll(own, k, 1) for k in (1, 2, 3)]
            from_high[pl.ds(v * ny, ny), :] = jnp.where(
                spot == 5, copies[0], jnp.where(spot == 6, copies[1], copies[2])
            )

    @pl.when(ms < n_stream - 1)
    def _():
        to_low.wait_recv()

    upper_side = lane < half
    edge = []
    for v in range(VARS):
        own = pack[pl.ds(v * ny, ny), :]
        low, high = from_low[pl.ds(v * ny, ny), :], from_high[pl.ds(v * ny, ny), :]
        edge.append(
            jnp.where(
                upper_side,
                jnp.where(spot < 5, own, high),
                jnp.where(spot < HALO, low, own),
            )
        )
    shifts = stream_shifts(edge)
    edge_left, edge_right = stream_states(shifts, edge)
    edge_faces = faces(edge_left, edge_right, shifts[1], edge, 0)
    middle = (spot >= HALO) & (spot < 2 * HALO)
    lo = [jnp.where(middle, f, 0.0) for f in edge_faces]
    hi = ahead(lo)
    merged = []
    for out in rate(lo, hi, edge[6]):
        upper = jnp.where(upper_side & (spot >= 2) & (spot < 5), out, 0.0)
        lower = jnp.where(jnp.logical_not(upper_side) & middle, out, 0.0)
        merged.append(upper + pltpu.roll(lower, nx - half + 2, 1))
    rim = (lane < HALO) | (lane >= nx - HALO)
    for z in range(cz):
        for v in range(VARS):
            patch = pltpu.roll(merged[v], (nx - HALO - 2 - GROUP * z) % nx, 1)
            rows = cell_rows(v, z)
            total[rows, :] = total[rows, :] + jnp.where(rim, patch, 0.0)
            kept[rows, :] = base[v, z] * (1.0 / 3.0) + (2.0 / 3.0) * now[v, z]

    halo_y[0].wait_recv()
    high_edge()

    if direct:

        @pl.when(early)
        def _():
            arrivals(top_first, size - 1, first_in)
            top = top_first[0]
            for d in range(1, size):
                top = jnp.maximum(top, top_first[d])
            mine[1] = top
            mine[2] = top

        @pl.when(caster)
        def _():
            for copy in cast:
                copy.start()

    halo_y[1].wait_recv()
    low_edge()

    for copy in halo_y:
        copy.wait_send()
    pl.when(outer)(to_high.wait_send)
    pl.when(inner)(to_low.wait_send)

    if direct:
        for h in range(HUBS):
            pl.when(jnp.logical_not(hubs[h]))(to_hub[h].wait_send)

        @pl.when(caster)
        def _():
            arrivals(top_first, len(cast), second_out)

        @pl.when(jnp.logical_not(early))
        def _():
            cast[0].wait_recv()

        top = mine[2]
    else:
        arrivals(top_first, len(across), first_out)
        arrivals(top_second, len(along), second_out)
        arrivals(top_second, len(along), second_in)
        top = mine[1]
        for d in range(len(along)):
            top = jnp.maximum(top, top_second[d])
    step = (2.0 / 3.0 * 0.3) / jnp.max(top, keepdims=True)
    scale[...] = jnp.broadcast_to(step, (ny, nx))


def finish(ny, kept, total, scale, out_ref):
    step = scale[...]
    for i in range(kept.shape[0] // ny):
        rows = pl.ds(i * ny, ny)
        out_ref[rows, :] = kept[rows, :] + step * total[rows, :]


def solution(mesh):
    n_stream, n_cross = mesh.shape["stream"], mesh.shape["cross"]
    direct = n_stream * n_cross <= DIRECT
    first = n_stream * n_cross if direct else n_cross - 1

    def shards(state_now, state_base, inflow):
        _, cz, ny, nx = state_now.shape
        f32 = jnp.float32
        vmem = lambda *shape: pltpu.VMEM(shape, f32)
        dma = lambda n: pltpu.SemaphoreType.DMA((n,))
        cells = VARS * cz * ny
        kept, total, scale = pl.pallas_call(
            functools.partial(kernel, (n_stream, n_cross, cz, ny, nx), direct),
            out_shape=(
                vmem(cells, nx),
                vmem(cells, nx),
                vmem(ny, nx),
            ),
            in_specs=[pl.BlockSpec(memory_space=pl.ANY)] * 3,
            out_specs=[pl.BlockSpec(memory_space=pltpu.VMEM)] * 3,
            scratch_shapes=[
                vmem(*state_now.shape),
                vmem(*state_now.shape),
                vmem(VARS, HALO, cz, ny),
                vmem(HALO, cz, nx),
                vmem(nx, nx),
                vmem((cz + 2 * HALO) * VARS * ny, nx),
                vmem((ny + 2 * HALO) * VARS * cz, nx),
                vmem(4, VARS, ny, nx),
                vmem(3, VARS, ny, nx),
                vmem(2, VARS + 1, ny, nx),
                vmem(VARS * ny, nx),
                vmem(VARS * ny, nx),
                vmem(VARS * ny, nx),
                vmem(4, VARS + 1, cz, nx),
                vmem(first, 1, nx),
                vmem(n_stream - 1, 1, nx),
                vmem(3, 1, nx),
                dma(3),
                dma(4),
                dma(4),
                dma(HUBS),
                dma(1),
                dma(1),
                dma(1),
            ],
            compiler_params=pltpu.CompilerParams(collective_id=0, has_side_effects=True),
        )(state_now, state_base, jnp.transpose(inflow, (0, 3, 1, 2)))
        kept, total, scale = [
            pltpu.with_memory_space_constraint(x, pltpu.VMEM) for x in (kept, total, scale)
        ]
        out = pl.pallas_call(
            functools.partial(finish, ny),
            out_shape=jax.ShapeDtypeStruct((cells, nx), f32),
            in_specs=[pl.BlockSpec(memory_space=pltpu.VMEM)] * 3,
            out_specs=pl.BlockSpec(memory_space=pltpu.VMEM),
        )(kept, total, scale)
        return out.reshape(state_now.shape)

    split = P(None, None, "cross", "stream")
    return jax.shard_map(
        shards,
        mesh=mesh,
        in_specs=(split, split, P(None, None, "cross", None)),
        out_specs=split,
        check_vma=False,
    )
```

```python
import functools

import jax
import jax.numpy as jnp
from jax import lax
from jax.experimental import pallas as pl
from jax.experimental.pallas import tpu as pltpu
from jax.sharding import PartitionSpec as P

MESH = pl.DeviceIdType.MESH
VARS = 7
HALO = 3
GROUP = 8
DIRECT = 64
HUBS = 2
STIFF = 4.4 * 0.6 / 3.4


def recip(x):
    return 1.0 / x


def mixture(volume):
    rest = 1.0 - volume
    return volume * (1.0 / 0.4) + rest * (1.0 / 3.4), rest * STIFF


def primitive(u):
    inv = recip(u[0] + u[1])
    vx, vy, vz = u[2] * inv, u[3] * inv, u[4] * inv
    gam, stiff = mixture(u[6])
    kinetic = 0.5 * (u[2] * vx + u[3] * vy + u[4] * vz)
    return [u[0], u[1], vx, vy, vz, (u[5] - kinetic - stiff) * recip(gam), u[6]]


def max_speed(w):
    gam, stiff = mixture(w[6])
    top = (gam + 1.0) * w[5] + stiff
    sound = jnp.sqrt(top * recip(gam * (w[0] + w[1])))
    return jnp.maximum(jnp.maximum(jnp.abs(w[2]), jnp.abs(w[3])), jnp.abs(w[4])) + sound


def weno_pair(f, g, h, k, l):
    e1, e2, e3, e4 = g - f, h - g, k - h, l - k
    s0, s1, s2 = e2 - e1, e3 - e2, e4 - e3
    d2, d3 = e2 + e2, e3 + e3
    t0, t1, t2 = d2 + s0, e2 + e3, d3 - s2
    eps = 1e-6 * 12.0 / 13.0
    r0 = recip(s0 * s0 + (eps + (3.0 / 13.0) * (t0 * t0)))
    r1 = recip(s1 * s1 + (eps + (3.0 / 13.0) * (t1 * t1)))
    r2 = recip(s2 * s2 + (eps + (3.0 / 13.0) * (t2 * t2)))
    a0, a1, a2 = r0 * r0, 6.0 * (r1 * r1), r2 * r2
    b0, b2 = 3.0 * a0, 3.0 * a2
    p0, p2 = t0 + e2, t2 + e3
    up = (a0 * (p0 + s0) + a1 * (d3 + e2) + b2 * p2) * recip(6.0 * (a0 + a1 + b2))
    down = (a2 * (p2 - s2) + a1 * (d2 + e3) + b0 * p0) * recip(6.0 * (a2 + a1 + b0))
    return h + up, h - down


def limit(state, low, high):
    out = list(state)
    for v in (0, 1, 5):
        out[v] = jnp.maximum(state[v], low[v])
    out[6] = jnp.minimum(jnp.maximum(state[6], low[6]), high)
    return out


def side(w, normal):
    dens = w[0] + w[1]
    gam, stiff = mixture(w[6])
    m = [dens * w[2], dens * w[3], dens * w[4]]
    heat = gam * w[5] + stiff
    energy = heat + 0.5 * (m[0] * w[2] + m[1] * w[3] + m[2] * w[4])
    vn = w[2 + normal]
    amounts = [w[0], w[1], m[0], m[1], m[2], energy, w[6]]
    moved = [q * vn for q in amounts]
    moved[2 + normal] = moved[2 + normal] + w[5]
    moved[5] = (energy + w[5]) * vn
    sound = jnp.sqrt((heat + w[5]) * recip(gam * dens))
    return amounts, moved, vn, jnp.abs(vn) + sound


def faces(left, right, below, above, normal):
    low = {v: 0.5 * jnp.minimum(below[v], above[v]) for v in (0, 1, 5, 6)}
    high = 1.0 - 0.5 * (1.0 - jnp.maximum(below[6], above[6]))
    ul, fl, nl, sl = side(limit(left, low, high), normal)
    ur, fr, nr, sr = side(limit(right, low, high), normal)
    fast = 0.5 * jnp.maximum(sl, sr)
    out = [0.5 * (fl[v] + fr[v]) - fast * (ur[v] - ul[v]) for v in range(VARS)]
    return out + [0.5 * (nl + nr)]


def rate(lo, hi, volume):
    out = [lo[v] - hi[v] for v in range(VARS)]
    out[6] = out[6] + volume * (hi[7] - lo[7])
    return out


def reader(src, height):
    def at(c, v):
        return src[pl.ds(pl.multiple_of((c * VARS + v) * height, height), height), :]

    def row(c):
        return [at(c, v) for v in range(VARS)]

    def states(c):
        pairs = [weno_pair(*[at(c + o, v) for o in range(-2, 3)]) for v in range(VARS)]
        return [p[0] for p in pairs], [p[1] for p in pairs]

    return at, row, states


def sweep(src, count, height, normal, emit):
    at, row, states = reader(src, height)

    def cell(c, left):
        after, right = states(c)
        return faces(left, right, row(c - 1), row(c), normal), after

    flux, left = cell(HALO, states(HALO - 1)[0])

    def step(i, carry):
        left, lo = carry
        hi, left = cell(i + HALO + 1, left)
        emit(i, rate(lo, hi, at(i + HALO, 6)))
        return left, hi

    lax.fori_loop(0, count, step, (left, flux))


def kernel(
    dims,
    direct,
    now_hbm,
    base_hbm,
    inflow_hbm,
    kept,
    total,
    scale,
    now,
    base,
    inflow,
    flat,
    wide,
    wz,
    wy,
    shifted,
    sided,
    fluxes,
    pack,
    from_low,
    from_high,
    joint,
    top_first,
    top_second,
    mine,
    load_sem,
    halo_send,
    halo_recv,
    first_send,
    first_recv,
    second_send,
    second_recv,
    ready_sem,
):
    n_stream, n_cross, cz, ny, nx = dims
    tile = VARS * ny
    ztile = VARS * cz
    half = cz * GROUP
    ms, mc = lax.axis_index("stream"), lax.axis_index("cross")

    loads = [
        pltpu.make_async_copy(base_hbm, base, load_sem.at[0]),
        pltpu.make_async_copy(now_hbm, now, load_sem.at[1]),
        pltpu.make_async_copy(inflow_hbm, inflow, load_sem.at[2]),
    ]
    for copy in loads:
        copy.start()

    size = n_stream * n_cross
    across = [(0, d) for d in range(1, n_cross)]
    along = [(d, 0) for d in range(1, n_stream)]
    others = [(d, e) for e in range(n_cross) for d in range(n_stream) if (d, e) != (0, 0)]
    inner, outer = ms > 0, ms < n_stream - 1
    lowest, highest = mc == 0, mc == n_cross - 1
    hubs = [(ms == h) & lowest for h in range(HUBS)]
    early = functools.reduce(jnp.logical_or, hubs)
    caster = hubs[HUBS - 1]

    def device(offset):
        return {
            "stream": lax.rem(ms + offset[0], n_stream),
            "cross": lax.rem(mc + offset[1], n_cross),
        }

    barrier = pltpu.get_barrier_semaphore()

    def greet(target):
        pl.semaphore_signal(barrier, device_id=target, device_id_type=MESH)

    above, below = device((0, 1)), device((0, n_cross - 1))
    after, before = device((1, 0)), device((n_stream - 1, 0))

    def ready(k, target):
        pl.semaphore_signal(ready_sem.at[k], device_id=target, device_id_type=MESH)

    def await_ready(k):
        pl.semaphore_wait(ready_sem.at[k], 1)

    if direct:
        pl.when(jnp.logical_not(highest))(lambda: greet(above))
        pl.when(lowest)(lambda: greet(below))
        pl.when(outer)(lambda: greet(after))

        @pl.when(early)
        def _():
            for p in others:
                greet(device(p))

        one = lambda flag: jnp.where(flag, 1, 0)
        greetings = jnp.where(early, HUBS - 1, HUBS)
        pl.semaphore_wait(
            barrier, greetings + one(inner) + one(highest) + one(jnp.logical_not(lowest))
        )
        pl.when(highest)(lambda: ready(2, above))
        pl.when(jnp.logical_not(lowest))(lambda: ready(0, below))
        pl.when(inner)(lambda: ready(1, before))
    else:
        for p in across + along:
            greet(device(p))
        pl.semaphore_wait(barrier, n_cross + n_stream - 2)

    def remote(src, dst, send, recv, target):
        return pltpu.make_async_remote_copy(
            src_ref=src,
            dst_ref=dst,
            send_sem=send,
            recv_sem=recv,
            device_id=target,
            device_id_type=MESH,
        )

    def spread(slot, buffer, offsets, send, recv):
        return [
            remote(mine.at[slot], buffer.at[i], send, recv, device(p))
            for i, p in enumerate(offsets)
        ]

    def arrivals(buffer, count, recv):
        part = buffer.at[pl.ds(0, count)]
        pltpu.make_async_copy(part, part, recv).wait()

    first_out, first_in = first_send.at[0], first_recv.at[0]
    second_out, second_in = second_send.at[0], second_recv.at[0]
    if direct:
        spot_here = ms * n_cross + mc
        to_hub = [
            remote(
                mine.at[0],
                top_first.at[spot_here],
                first_send.at[h],
                first_in,
                {"stream": h, "cross": 0},
            )
            for h in range(HUBS)
        ]
        cast = [
            remote(mine.at[1], mine.at[2], second_out, second_in, {"stream": d, "cross": e})
            for e in range(n_cross)
            for d in range(n_stream)
            if e > 0 or d >= HUBS
        ]
    else:
        first = spread(0, top_first, across, first_out, first_in)
        second = spread(1, top_second, along, second_out, second_in)

    def send_speed():
        if direct:
            for h in range(HUBS):
                pl.when(jnp.logical_not(hubs[h]))(to_hub[h].start)
        else:
            for copy in first:
                copy.start()

    rows = HALO * ztile
    halo_y = [
        pltpu.make_async_remote_copy(
            src_ref=wy.at[pl.ds(rows, rows)],
            dst_ref=wy.at[pl.ds((HALO + ny) * ztile, rows)],
            send_sem=halo_send.at[0],
            recv_sem=halo_recv.at[0],
            device_id=below,
            device_id_type=MESH,
        ),
        pltpu.make_async_remote_copy(
            src_ref=wy.at[pl.ds(ny * ztile, rows)],
            dst_ref=wy.at[pl.ds(0, rows)],
            send_sem=halo_send.at[1],
            recv_sem=halo_recv.at[1],
            device_id=above,
            device_id_type=MESH,
        ),
    ]
    to_high = pltpu.make_async_remote_copy(
        src_ref=pack,
        dst_ref=from_low,
        send_sem=halo_send.at[2],
        recv_sem=halo_recv.at[2],
        device_id=after,
        device_id_type=MESH,
    )
    to_low = pltpu.make_async_remote_copy(
        src_ref=pack,
        dst_ref=from_high,
        send_sem=halo_send.at[3],
        recv_sem=halo_recv.at[3],
        device_id=before,
        device_id_type=MESH,
    )

    def send_up():
        halo_y[1].start()

    def send_up_ready():
        await_ready(0)
        halo_y[1].start()

    def send_down():
        halo_y[0].start()

    def send_down_around():
        await_ready(2)
        halo_y[0].start()

    def send_after():
        if direct:
            await_ready(1)
        to_high.start()

    def by_plane(y):
        for v in range(VARS):
            wy[pl.ds((HALO + y) * ztile + v * cz, cz), :] = wz[
                pl.ds(HALO * tile + v * ny + y, cz, stride=tile), :
            ]

    loads[0].wait()
    speed = None
    for z in range(cz):
        s = max_speed(primitive([base[v, z] for v in range(VARS)]))
        speed = s if speed is None else jnp.maximum(speed, s)
    mine[0] = jnp.max(speed, axis=0, keepdims=True)
    if direct:
        top_first[spot_here] = mine[0]
    send_speed()

    loads[1].wait()
    lane = lax.broadcasted_iota(jnp.int32, (ny, nx), 1)
    group = lane // GROUP
    for z in range(cz):
        w = primitive([now[v, z] for v in range(VARS)])
        spots = [HALO + z]
        if z < HALO:
            spots.append(HALO + cz + z)
        if z >= cz - HALO:
            spots.append(z - (cz - HALO))
        for v in range(VARS):
            for c in spots:
                wz[pl.ds(c * tile + v * ny, ny), :] = w[v]
    for y in range(ny):
        by_plane(y)
    if direct:
        pl.when(highest)(send_up)
        pl.when(jnp.logical_not(highest | lowest))(send_down)
    else:
        send_up()
        send_down()

    for v in range(VARS):
        packed = None
        for z in range(cz):
            w = wz[pl.ds((HALO + z) * tile + v * ny, ny), :]
            upper = pltpu.roll(w, (GROUP * z - (nx - 5)) % nx, 1)
            lower = pltpu.roll(w, (half + GROUP * z + HALO) % nx, 1)
            piece = jnp.where(group == z, upper, lower)
            if z == 0:
                packed = piece
            else:
                packed = jnp.where((group == z) | (group == cz + z), piece, packed)
        pack[pl.ds(v * ny, ny), :] = packed
    pl.when(inner)(to_low.start)

    def stream_shifts(w):
        return [[pltpu.roll(x, d % nx, 1) for x in w] for d in (2, 1, -1, -2)]

    def stream_states(shifts, w):
        m2, m1, p1, p2 = shifts
        pairs = [weno_pair(m2[v], m1[v], w[v], p1[v], p2[v]) for v in range(VARS)]
        return [pltpu.roll(p[0], 1, 1) for p in pairs], [p[1] for p in pairs]

    def ahead(lo):
        return [pltpu.roll(f, nx - 1, 1) for f in lo]

    def cell_rows(v, z):
        return pl.ds(pl.multiple_of((v * cz + z) * ny, ny), ny)

    def keep_rate(z, out):
        for v in range(VARS):
            total[cell_rows(v, z), :] = out[v]

    sweep(wz, cz, ny, 2, keep_rate)

    pl.when(outer)(send_after)
    if direct:
        pl.when(jnp.logical_not(highest))(send_up_ready)

    whole = (lane >= HALO) & (lane < nx - 2)

    def centre(z):
        return [
            wz[pl.ds(pl.multiple_of(((HALO + z) * VARS + v) * ny, ny), ny), :]
            for v in range(VARS)
        ]

    def stage_shift(z):
        for d, row in enumerate(stream_shifts(centre(z))):
            for v in range(VARS):
                shifted[d, v] = row[v]

    def stage_state(z):
        shifts = [[shifted[d, v] for v in range(VARS)] for d in range(4)]
        left, right = stream_states(shifts, centre(z))
        for v in range(VARS):
            sided[0, v] = left[v]
            sided[1, v] = right[v]
            sided[2, v] = shifts[1][v]

    def stage_flux(z):
        left, right, below = [[sided[k, v] for v in range(VARS)] for k in range(3)]
        lo = [jnp.where(whole, f, 0.0) for f in faces(left, right, below, centre(z), 0)]
        hi = ahead(lo)
        for o in range(VARS + 1):
            fluxes[0, o] = lo[o]
            fluxes[1, o] = hi[o]

    def stage_rate(z):
        lo, hi = [[fluxes[k, o] for o in range(VARS + 1)] for k in range(2)]
        out = rate(lo, hi, centre(z)[6])
        for v in range(VARS):
            total[cell_rows(v, z), :] = total[cell_rows(v, z), :] + out[v]

    stages = (stage_shift, stage_state, stage_flux, stage_rate)
    depth = len(stages)

    def advance(z):
        for k in reversed(range(depth)):
            stages[k](z - k)

    for z in range(depth - 1):
        for k in reversed(range(z + 1)):
            stages[k](z - k)
    lax.fori_loop(depth - 1, cz, lambda z, c: (advance(z), c)[1], 0)
    for z in range(cz, cz + depth - 1):
        for k in reversed(range(z - cz + 1, depth)):
            stages[k](z - k)

    if direct:
        pl.when(highest)(send_down)

    def add_rate(y, out):
        for v in range(VARS):
            rows = pl.ds(v * cz * ny + y, cz, stride=ny)
            total[rows, :] = total[rows, :] + out[v]

    wy_at, wy_row, wy_states = reader(wy, cz)

    def cross_face(y, left, right):
        return faces(left, right, wy_row(HALO + y - 1), wy_row(HALO + y), 1)

    def cross_rate(y, lo, hi):
        add_rate(y, rate(lo, hi, wy_at(HALO + y, 6)))

    def save(slot, values):
        for k, x in enumerate(values):
            joint[slot, k] = x

    def saved(slot, size):
        return [joint[slot, k] for k in range(size)]

    left, right = wy_states(2 * HALO - 1)
    save(0, right)
    lo = None
    for y in range(HALO, ny - HALO + 1):
        after, right = wy_states(HALO + y)
        hi = cross_face(y, left, right)
        if lo is None:
            save(1, hi)
        else:
            cross_rate(y - 1, lo, hi)
        left, lo = after, hi
    save(2, left)
    save(3, lo)

    def low_edge():
        left, _ = wy_states(HALO - 1)
        lo = None
        for y in range(HALO):
            if y < HALO - 1:
                after, right = wy_states(HALO + y)
            else:
                after, right = None, saved(0, VARS)
            hi = cross_face(y, left, right)
            if lo is not None:
                cross_rate(y - 1, lo, hi)
            left, lo = after, hi
        cross_rate(HALO - 1, lo, saved(1, VARS + 1))

    def high_edge():
        left, lo = saved(2, VARS), saved(3, VARS + 1)
        for y in range(ny - HALO + 1, ny + 1):
            after, right = wy_states(HALO + y)
            hi = cross_face(y, left, right)
            cross_rate(y - 1, lo, hi)
            left, lo = after, hi

    if not direct:
        arrivals(top_first, len(across), first_in)
        slab = mine[0]
        for d in range(len(across)):
            slab = jnp.maximum(slab, top_first[d])
        mine[1] = slab
        for copy in second:
            copy.start()

    loads[2].wait()

    @pl.when(ms == 0)
    def _():
        for k in range(HALO):
            for v in range(VARS):
                flat[k, :, pl.ds(v * ny, ny)] = inflow[v, k]
            wide[pl.ds(half + k, cz, stride=GROUP), :] = flat[k]
        turned = jnp.transpose(wide[...])
        w = primitive([turned[v * ny : (v + 1) * ny] for v in range(VARS)])
        for v in range(VARS):
            from_low[pl.ds(v * ny, ny), :] = w[v]

    @pl.when(ms > 0)
    def _():
        to_high.wait_recv()

    spot = lane % GROUP

    @pl.when(ms == n_stream - 1)
    def _():
        for v in range(VARS):
            own = pack[pl.ds(v * ny, ny), :]
            copies = [pltpu.roll(own, k, 1) for k in (1, 2, 3)]
            from_high[pl.ds(v * ny, ny), :] = jnp.where(
                spot == 5, copies[0], jnp.where(spot == 6, copies[1], copies[2])
            )

    @pl.when(ms < n_stream - 1)
    def _():
        to_low.wait_recv()

    upper_side = lane < half
    edge = []
    for v in range(VARS):
        own = pack[pl.ds(v * ny, ny), :]
        low, high = from_low[pl.ds(v * ny, ny), :], from_high[pl.ds(v * ny, ny), :]
        edge.append(
            jnp.where(
                upper_side,
                jnp.where(spot < 5, own, high),
                jnp.where(spot < HALO, low, own),
            )
        )
    shifts = stream_shifts(edge)
    edge_left, edge_right = stream_states(shifts, edge)
    edge_faces = faces(edge_left, edge_right, shifts[1], edge, 0)
    middle = (spot >= HALO) & (spot < 2 * HALO)
    lo = [jnp.where(middle, f, 0.0) for f in edge_faces]
    hi = ahead(lo)
    merged = []
    for out in rate(lo, hi, edge[6]):
        upper = jnp.where(upper_side & (spot >= 2) & (spot < 5), out, 0.0)
        lower = jnp.where(jnp.logical_not(upper_side) & middle, out, 0.0)
        merged.append(upper + pltpu.roll(lower, nx - half + 2, 1))
    rim = (lane < HALO) | (lane >= nx - HALO)
    for z in range(cz):
        for v in range(VARS):
            patch = pltpu.roll(merged[v], (nx - HALO - 2 - GROUP * z) % nx, 1)
            rows = cell_rows(v, z)
            total[rows, :] = total[rows, :] + jnp.where(rim, patch, 0.0)
            kept[rows, :] = base[v, z] * (1.0 / 3.0) + (2.0 / 3.0) * now[v, z]

    if direct:
        pl.when(lowest)(send_down_around)
    halo_y[0].wait_recv()
    high_edge()

    if direct:

        @pl.when(early)
        def _():
            arrivals(top_first, size - 1, first_in)
            top = top_first[0]
            for d in range(1, size):
                top = jnp.maximum(top, top_first[d])
            mine[1] = top
            mine[2] = top

        @pl.when(caster)
        def _():
            for copy in cast:
                copy.start()

    halo_y[1].wait_recv()
    low_edge()

    for copy in halo_y:
        copy.wait_send()
    pl.when(outer)(to_high.wait_send)
    pl.when(inner)(to_low.wait_send)

    if direct:
        for h in range(HUBS):
            pl.when(jnp.logical_not(hubs[h]))(to_hub[h].wait_send)

        @pl.when(caster)
        def _():
            arrivals(top_first, len(cast), second_out)

        @pl.when(jnp.logical_not(early))
        def _():
            cast[0].wait_recv()

        top = mine[2]
    else:
        arrivals(top_first, len(across), first_out)
        arrivals(top_second, len(along), second_out)
        arrivals(top_second, len(along), second_in)
        top = mine[1]
        for d in range(len(along)):
            top = jnp.maximum(top, top_second[d])
    step = (2.0 / 3.0 * 0.3) / jnp.max(top, keepdims=True)
    scale[...] = jnp.broadcast_to(step, (ny, nx))


def finish(ny, kept, total, scale, out_ref):
    step = scale[...]
    for i in range(kept.shape[0] // ny):
        rows = pl.ds(i * ny, ny)
        out_ref[rows, :] = kept[rows, :] + step * total[rows, :]


def solution(mesh):
    n_stream, n_cross = mesh.shape["stream"], mesh.shape["cross"]
    direct = n_stream * n_cross <= DIRECT
    first = n_stream * n_cross if direct else n_cross - 1

    def shards(state_now, state_base, inflow):
        _, cz, ny, nx = state_now.shape
        f32 = jnp.float32
        vmem = lambda *shape: pltpu.VMEM(shape, f32)
        dma = lambda n: pltpu.SemaphoreType.DMA((n,))
        cells = VARS * cz * ny
        kept, total, scale = pl.pallas_call(
            functools.partial(kernel, (n_stream, n_cross, cz, ny, nx), direct),
            out_shape=(
                vmem(cells, nx),
                vmem(cells, nx),
                vmem(ny, nx),
            ),
            in_specs=[pl.BlockSpec(memory_space=pl.ANY)] * 3,
            out_specs=[pl.BlockSpec(memory_space=pltpu.VMEM)] * 3,
            scratch_shapes=[
                vmem(*state_now.shape),
                vmem(*state_now.shape),
                vmem(VARS, HALO, cz, ny),
                vmem(HALO, cz, nx),
                vmem(nx, nx),
                vmem((cz + 2 * HALO) * VARS * ny, nx),
                vmem((ny + 2 * HALO) * VARS * cz, nx),
                vmem(4, VARS, ny, nx),
                vmem(3, VARS, ny, nx),
                vmem(2, VARS + 1, ny, nx),
                vmem(VARS * ny, nx),
                vmem(VARS * ny, nx),
                vmem(VARS * ny, nx),
                vmem(4, VARS + 1, cz, nx),
                vmem(first, 1, nx),
                vmem(n_stream - 1, 1, nx),
                vmem(3, 1, nx),
                dma(3),
                dma(4),
                dma(4),
                dma(HUBS),
                dma(1),
                dma(1),
                dma(1),
                pltpu.SemaphoreType.REGULAR((3,)),
            ],
            compiler_params=pltpu.CompilerParams(collective_id=0, has_side_effects=True),
        )(state_now, state_base, jnp.transpose(inflow, (0, 3, 1, 2)))
        kept, total, scale = [
            pltpu.with_memory_space_constraint(x, pltpu.VMEM) for x in (kept, total, scale)
        ]
        out = pl.pallas_call(
            functools.partial(finish, ny),
            out_shape=jax.ShapeDtypeStruct((cells, nx), f32),
            in_specs=[pl.BlockSpec(memory_space=pltpu.VMEM)] * 3,
            out_specs=pl.BlockSpec(memory_space=pltpu.VMEM),
        )(kept, total, scale)
        return out.reshape(state_now.shape)

    split = P(None, None, "cross", "stream")
    return jax.shard_map(
        shards,
        mesh=mesh,
        in_specs=(split, split, P(None, None, "cross", None)),
        out_specs=split,
        check_vma=False,
    )
```

```python
import functools

import jax
import jax.numpy as jnp
from jax import lax
from jax.experimental import pallas as pl
from jax.experimental.pallas import tpu as pltpu
from jax.sharding import PartitionSpec as P

MESH = pl.DeviceIdType.MESH
VARS = 7
HALO = 3
GROUP = 8
DIRECT = 64
HUBS = 2
STIFF = 4.4 * 0.6 / 3.4


def recip(x):
    return 1.0 / x


def mixture(volume):
    rest = 1.0 - volume
    return volume * (1.0 / 0.4) + rest * (1.0 / 3.4), rest * STIFF


def primitive(u):
    inv = recip(u[0] + u[1])
    vx, vy, vz = u[2] * inv, u[3] * inv, u[4] * inv
    gam, stiff = mixture(u[6])
    kinetic = 0.5 * (u[2] * vx + u[3] * vy + u[4] * vz)
    return [u[0], u[1], vx, vy, vz, (u[5] - kinetic - stiff) * recip(gam), u[6]]


def max_speed(w):
    gam, stiff = mixture(w[6])
    top = (gam + 1.0) * w[5] + stiff
    sound = jnp.sqrt(top * recip(gam * (w[0] + w[1])))
    return jnp.maximum(jnp.maximum(jnp.abs(w[2]), jnp.abs(w[3])), jnp.abs(w[4])) + sound


def weno_pair(f, g, h, k, l):
    e1, e2, e3, e4 = g - f, h - g, k - h, l - k
    s0, s1, s2 = e2 - e1, e3 - e2, e4 - e3
    d2, d3 = e2 + e2, e3 + e3
    t0, t1, t2 = d2 + s0, e2 + e3, d3 - s2
    eps = 1e-6 * 12.0 / 13.0
    r0 = recip(s0 * s0 + (eps + (3.0 / 13.0) * (t0 * t0)))
    r1 = recip(s1 * s1 + (eps + (3.0 / 13.0) * (t1 * t1)))
    r2 = recip(s2 * s2 + (eps + (3.0 / 13.0) * (t2 * t2)))
    a0, a1, a2 = r0 * r0, 6.0 * (r1 * r1), r2 * r2
    b0, b2 = 3.0 * a0, 3.0 * a2
    p0, p2 = t0 + e2, t2 + e3
    up = (a0 * (p0 + s0) + a1 * (d3 + e2) + b2 * p2) * recip(6.0 * (a0 + a1 + b2))
    down = (a2 * (p2 - s2) + a1 * (d2 + e3) + b0 * p0) * recip(6.0 * (a2 + a1 + b0))
    return h + up, h - down


def limit(state, low, high):
    out = list(state)
    for v in (0, 1, 5):
        out[v] = jnp.maximum(state[v], low[v])
    out[6] = jnp.minimum(jnp.maximum(state[6], low[6]), high)
    return out


def side(w, normal):
    dens = w[0] + w[1]
    gam, stiff = mixture(w[6])
    m = [dens * w[2], dens * w[3], dens * w[4]]
    heat = gam * w[5] + stiff
    energy = heat + 0.5 * (m[0] * w[2] + m[1] * w[3] + m[2] * w[4])
    vn = w[2 + normal]
    amounts = [w[0], w[1], m[0], m[1], m[2], energy, w[6]]
    moved = [q * vn for q in amounts]
    moved[2 + normal] = moved[2 + normal] + w[5]
    moved[5] = (energy + w[5]) * vn
    sound = jnp.sqrt((heat + w[5]) * recip(gam * dens))
    return amounts, moved, vn, jnp.abs(vn) + sound


def faces(left, right, below, above, normal):
    low = {v: 0.5 * jnp.minimum(below[v], above[v]) for v in (0, 1, 5, 6)}
    high = 1.0 - 0.5 * (1.0 - jnp.maximum(below[6], above[6]))
    ul, fl, nl, sl = side(limit(left, low, high), normal)
    ur, fr, nr, sr = side(limit(right, low, high), normal)
    fast = 0.5 * jnp.maximum(sl, sr)
    out = [0.5 * (fl[v] + fr[v]) - fast * (ur[v] - ul[v]) for v in range(VARS)]
    return out + [0.5 * (nl + nr)]


def rate(lo, hi, volume):
    out = [lo[v] - hi[v] for v in range(VARS)]
    out[6] = out[6] + volume * (hi[7] - lo[7])
    return out


def reader(src, height):
    def at(c, v):
        return src[pl.ds(pl.multiple_of((c * VARS + v) * height, height), height), :]

    def row(c):
        return [at(c, v) for v in range(VARS)]

    def states(c):
        pairs = [weno_pair(*[at(c + o, v) for o in range(-2, 3)]) for v in range(VARS)]
        return [p[0] for p in pairs], [p[1] for p in pairs]

    return at, row, states


def sweep(src, count, height, normal, emit):
    at, row, states = reader(src, height)

    def cell(c, left):
        after, right = states(c)
        return faces(left, right, row(c - 1), row(c), normal), after

    flux, left = cell(HALO, states(HALO - 1)[0])

    def step(i, carry):
        left, lo = carry
        hi, left = cell(i + HALO + 1, left)
        emit(i, rate(lo, hi, at(i + HALO, 6)))
        return left, hi

    lax.fori_loop(0, count, step, (left, flux))


def kernel(
    dims,
    direct,
    now_hbm,
    base_hbm,
    inflow_hbm,
    kept,
    total,
    scale,
    now,
    base,
    inflow,
    flat,
    wide,
    wz,
    wy,
    shifted,
    sided,
    fluxes,
    pack,
    from_low,
    from_high,
    joint,
    top_first,
    top_second,
    mine,
    load_sem,
    halo_send,
    halo_recv,
    first_send,
    first_recv,
    second_send,
    second_recv,
    ready_sem,
):
    n_stream, n_cross, cz, ny, nx = dims
    tile = VARS * ny
    ztile = VARS * cz
    half = cz * GROUP
    ms, mc = lax.axis_index("stream"), lax.axis_index("cross")

    loads = [
        pltpu.make_async_copy(base_hbm, base, load_sem.at[0]),
        pltpu.make_async_copy(now_hbm, now, load_sem.at[1]),
        pltpu.make_async_copy(inflow_hbm, inflow, load_sem.at[2]),
    ]
    for v in range(VARS):
        pltpu.make_async_copy(base_hbm.at[v], base.at[v], load_sem.at[0]).start()
    for v in range(VARS):
        pltpu.make_async_copy(now_hbm.at[v], now.at[v], load_sem.at[1]).start()
    loads[2].start()

    size = n_stream * n_cross
    across = [(0, d) for d in range(1, n_cross)]
    along = [(d, 0) for d in range(1, n_stream)]
    others = [(d, e) for e in range(n_cross) for d in range(n_stream) if (d, e) != (0, 0)]
    inner, outer = ms > 0, ms < n_stream - 1
    lowest, highest = mc == 0, mc == n_cross - 1
    hubs = [(ms == h) & lowest for h in range(HUBS)]
    early = functools.reduce(jnp.logical_or, hubs)
    caster = hubs[HUBS - 1]

    def device(offset):
        return {
            "stream": lax.rem(ms + offset[0], n_stream),
            "cross": lax.rem(mc + offset[1], n_cross),
        }

    barrier = pltpu.get_barrier_semaphore()

    def greet(target):
        pl.semaphore_signal(barrier, device_id=target, device_id_type=MESH)

    above, below = device((0, 1)), device((0, n_cross - 1))
    after, before = device((1, 0)), device((n_stream - 1, 0))

    def ready(k, target):
        pl.semaphore_signal(ready_sem.at[k], device_id=target, device_id_type=MESH)

    def await_ready(k):
        pl.semaphore_wait(ready_sem.at[k], 1)

    if direct:
        pl.when(jnp.logical_not(highest))(lambda: greet(above))
        pl.when(lowest)(lambda: greet(below))
        pl.when(outer)(lambda: greet(after))

        @pl.when(early)
        def _():
            for p in others:
                greet(device(p))

        one = lambda flag: jnp.where(flag, 1, 0)
        greetings = jnp.where(early, HUBS - 1, HUBS)
        pl.semaphore_wait(
            barrier, greetings + one(inner) + one(highest) + one(jnp.logical_not(lowest))
        )
        pl.when(highest)(lambda: ready(2, above))
        pl.when(jnp.logical_not(lowest))(lambda: ready(0, below))
        pl.when(inner)(lambda: ready(1, before))
    else:
        for p in across + along:
            greet(device(p))
        pl.semaphore_wait(barrier, n_cross + n_stream - 2)

    def remote(src, dst, send, recv, target):
        return pltpu.make_async_remote_copy(
            src_ref=src,
            dst_ref=dst,
            send_sem=send,
            recv_sem=recv,
            device_id=target,
            device_id_type=MESH,
        )

    def spread(slot, buffer, offsets, send, recv):
        return [
            remote(mine.at[slot], buffer.at[i], send, recv, device(p))
            for i, p in enumerate(offsets)
        ]

    def arrivals(buffer, count, recv):
        part = buffer.at[pl.ds(0, count)]
        pltpu.make_async_copy(part, part, recv).wait()

    first_out, first_in = first_send.at[0], first_recv.at[0]
    second_out, second_in = second_send.at[0], second_recv.at[0]
    if direct:
        spot_here = ms * n_cross + mc
        to_hub = [
            remote(
                mine.at[0],
                top_first.at[spot_here],
                first_send.at[h],
                first_in,
                {"stream": h, "cross": 0},
            )
            for h in range(HUBS)
        ]
        cast = [
            remote(mine.at[1], mine.at[2], second_out, second_in, {"stream": d, "cross": e})
            for e in range(n_cross)
            for d in range(n_stream)
            if e > 0 or d >= HUBS
        ]
    else:
        first = spread(0, top_first, across, first_out, first_in)
        second = spread(1, top_second, along, second_out, second_in)

    def send_speed():
        if direct:
            for h in range(HUBS):
                pl.when(jnp.logical_not(hubs[h]))(to_hub[h].start)
        else:
            for copy in first:
                copy.start()

    rows = HALO * ztile
    down = remote(
        wy.at[pl.ds(rows, rows)],
        wy.at[pl.ds((HALO + ny) * ztile, rows)],
        halo_send.at[0],
        halo_recv.at[0],
        below,
    )
    up = [
        remote(
            wy.at[pl.ds((ny + k) * ztile, ztile)],
            wy.at[pl.ds(k * ztile, ztile)],
            halo_send.at[3 + k],
            halo_recv.at[3 + k],
            above,
        )
        for k in range(HALO)
    ]
    to_high = pltpu.make_async_remote_copy(
        src_ref=pack,
        dst_ref=from_low,
        send_sem=halo_send.at[1],
        recv_sem=halo_recv.at[1],
        device_id=after,
        device_id_type=MESH,
    )
    to_low = pltpu.make_async_remote_copy(
        src_ref=pack,
        dst_ref=from_high,
        send_sem=halo_send.at[2],
        recv_sem=halo_recv.at[2],
        device_id=before,
        device_id_type=MESH,
    )

    def send_up():
        for copy in reversed(up):
            copy.start()

    def send_up_ready():
        await_ready(0)
        send_up()

    def send_down():
        down.start()

    def send_down_around():
        await_ready(2)
        down.start()

    def send_after():
        if direct:
            await_ready(1)
        to_high.start()

    def by_plane(y):
        for v in range(VARS):
            wy[pl.ds((HALO + y) * ztile + v * cz, cz), :] = wz[
                pl.ds(HALO * tile + v * ny + y, cz, stride=tile), :
            ]

    loads[0].wait()
    speed = None
    for z in range(cz):
        s = max_speed(primitive([base[v, z] for v in range(VARS)]))
        speed = s if speed is None else jnp.maximum(speed, s)
    mine[0] = jnp.max(speed, axis=0, keepdims=True)
    if direct:
        top_first[spot_here] = mine[0]
    send_speed()

    loads[1].wait()
    lane = lax.broadcasted_iota(jnp.int32, (ny, nx), 1)
    group = lane // GROUP
    for z in range(cz):
        w = primitive([now[v, z] for v in range(VARS)])
        spots = [HALO + z]
        if z < HALO:
            spots.append(HALO + cz + z)
        if z >= cz - HALO:
            spots.append(z - (cz - HALO))
        for v in range(VARS):
            for c in spots:
                wz[pl.ds(c * tile + v * ny, ny), :] = w[v]
    for y in range(ny):
        by_plane(y)
    if direct:
        pl.when(highest)(send_up)
        pl.when(jnp.logical_not(highest | lowest))(send_down)
    else:
        send_up()
        send_down()

    for v in range(VARS):
        packed = None
        for z in range(cz):
            w = wz[pl.ds((HALO + z) * tile + v * ny, ny), :]
            upper = pltpu.roll(w, (GROUP * z - (nx - 5)) % nx, 1)
            lower = pltpu.roll(w, (half + GROUP * z + HALO) % nx, 1)
            piece = jnp.where(group == z, upper, lower)
            if z == 0:
                packed = piece
            else:
                packed = jnp.where((group == z) | (group == cz + z), piece, packed)
        pack[pl.ds(v * ny, ny), :] = packed
    pl.when(inner)(to_low.start)

    def stream_shifts(w):
        return [[pltpu.roll(x, d % nx, 1) for x in w] for d in (2, 1, -1, -2)]

    def stream_states(shifts, w):
        m2, m1, p1, p2 = shifts
        pairs = [weno_pair(m2[v], m1[v], w[v], p1[v], p2[v]) for v in range(VARS)]
        return [pltpu.roll(p[0], 1, 1) for p in pairs], [p[1] for p in pairs]

    def ahead(lo):
        return [pltpu.roll(f, nx - 1, 1) for f in lo]

    def cell_rows(v, z):
        return pl.ds(pl.multiple_of((v * cz + z) * ny, ny), ny)

    def keep_rate(z, out):
        for v in range(VARS):
            total[cell_rows(v, z), :] = out[v]

    sweep(wz, cz, ny, 2, keep_rate)

    pl.when(outer)(send_after)
    if direct:
        pl.when(jnp.logical_not(highest))(send_up_ready)

    whole = (lane >= HALO) & (lane < nx - 2)

    def centre(z):
        return [
            wz[pl.ds(pl.multiple_of(((HALO + z) * VARS + v) * ny, ny), ny), :]
            for v in range(VARS)
        ]

    def stage_shift(z):
        for d, row in enumerate(stream_shifts(centre(z))):
            for v in range(VARS):
                shifted[d, v] = row[v]

    def stage_state(z):
        shifts = [[shifted[d, v] for v in range(VARS)] for d in range(4)]
        left, right = stream_states(shifts, centre(z))
        for v in range(VARS):
            sided[0, v] = left[v]
            sided[1, v] = right[v]
            sided[2, v] = shifts[1][v]

    def stage_flux(z):
        left, right, below = [[sided[k, v] for v in range(VARS)] for k in range(3)]
        lo = [jnp.where(whole, f, 0.0) for f in faces(left, right, below, centre(z), 0)]
        hi = ahead(lo)
        for o in range(VARS + 1):
            fluxes[0, o] = lo[o]
            fluxes[1, o] = hi[o]

    def stage_rate(z):
        lo, hi = [[fluxes[k, o] for o in range(VARS + 1)] for k in range(2)]
        out = rate(lo, hi, centre(z)[6])
        for v in range(VARS):
            total[cell_rows(v, z), :] = total[cell_rows(v, z), :] + out[v]

    stages = (stage_shift, stage_state, stage_flux, stage_rate)
    depth = len(stages)

    def advance(z):
        for k in reversed(range(depth)):
            stages[k](z - k)

    for z in range(depth - 1):
        for k in reversed(range(z + 1)):
            stages[k](z - k)
    lax.fori_loop(depth - 1, cz, lambda z, c: (advance(z), c)[1], 0)
    for z in range(cz, cz + depth - 1):
        for k in reversed(range(z - cz + 1, depth)):
            stages[k](z - k)

    if direct:
        pl.when(highest)(send_down)

    def add_rate(y, out):
        for v in range(VARS):
            rows = pl.ds(v * cz * ny + y, cz, stride=ny)
            total[rows, :] = total[rows, :] + out[v]

    wy_at, wy_row, wy_states = reader(wy, cz)

    def cross_face(y, left, right):
        return faces(left, right, wy_row(HALO + y - 1), wy_row(HALO + y), 1)

    def cross_rate(y, lo, hi):
        add_rate(y, rate(lo, hi, wy_at(HALO + y, 6)))

    def save(slot, values):
        for k, x in enumerate(values):
            joint[slot, k] = x

    def saved(slot, size):
        return [joint[slot, k] for k in range(size)]

    left, right = wy_states(2 * HALO - 1)
    save(0, right)
    lo = None
    for y in range(HALO, ny - HALO + 1):
        after, right = wy_states(HALO + y)
        hi = cross_face(y, left, right)
        if lo is None:
            save(1, hi)
        else:
            cross_rate(y - 1, lo, hi)
        left, lo = after, hi
    save(2, left)
    save(3, lo)

    def low_edge(cells, joint_in, joint_out):
        ahead_flux, next_right = saved(joint_in[1], VARS + 1), saved(joint_in[0], VARS)
        for y in cells:
            up[y].wait_recv()
            left, right = wy_states(HALO + y - 1)
            lo = cross_face(y, left, next_right)
            cross_rate(y, lo, ahead_flux)
            ahead_flux, next_right = lo, right
        if joint_out:
            save(joint_out[0], next_right)
            save(joint_out[1], ahead_flux)

    def high_edge():
        left, lo = saved(2, VARS), saved(3, VARS + 1)
        for y in range(ny - HALO + 1, ny + 1):
            after, right = wy_states(HALO + y)
            hi = cross_face(y, left, right)
            cross_rate(y - 1, lo, hi)
            left, lo = after, hi

    if not direct:
        arrivals(top_first, len(across), first_in)
        slab = mine[0]
        for d in range(len(across)):
            slab = jnp.maximum(slab, top_first[d])
        mine[1] = slab
        for copy in second:
            copy.start()

    loads[2].wait()

    @pl.when(ms == 0)
    def _():
        for k in range(HALO):
            for v in range(VARS):
                flat[k, :, pl.ds(v * ny, ny)] = inflow[v, k]
            wide[pl.ds(half + k, cz, stride=GROUP), :] = flat[k]
        turned = jnp.transpose(wide[...])
        w = primitive([turned[v * ny : (v + 1) * ny] for v in range(VARS)])
        for v in range(VARS):
            from_low[pl.ds(v * ny, ny), :] = w[v]

    @pl.when(ms > 0)
    def _():
        to_high.wait_recv()

    spot = lane % GROUP

    @pl.when(ms == n_stream - 1)
    def _():
        for v in range(VARS):
            own = pack[pl.ds(v * ny, ny), :]
            copies = [pltpu.roll(own, k, 1) for k in (1, 2, 3)]
            from_high[pl.ds(v * ny, ny), :] = jnp.where(
                spot == 5, copies[0], jnp.where(spot == 6, copies[1], copies[2])
            )

    @pl.when(ms < n_stream - 1)
    def _():
        to_low.wait_recv()

    upper_side = lane < half
    edge = []
    for v in range(VARS):
        own = pack[pl.ds(v * ny, ny), :]
        low, high = from_low[pl.ds(v * ny, ny), :], from_high[pl.ds(v * ny, ny), :]
        edge.append(
            jnp.where(
                upper_side,
                jnp.where(spot < 5, own, high),
                jnp.where(spot < HALO, low, own),
            )
        )
    shifts = stream_shifts(edge)
    edge_left, edge_right = stream_states(shifts, edge)
    edge_faces = faces(edge_left, edge_right, shifts[1], edge, 0)
    middle = (spot >= HALO) & (spot < 2 * HALO)
    lo = [jnp.where(middle, f, 0.0) for f in edge_faces]
    hi = ahead(lo)
    merged = []
    for out in rate(lo, hi, edge[6]):
        upper = jnp.where(upper_side & (spot >= 2) & (spot < 5), out, 0.0)
        lower = jnp.where(jnp.logical_not(upper_side) & middle, out, 0.0)
        merged.append(upper + pltpu.roll(lower, nx - half + 2, 1))
    rim = (lane < HALO) | (lane >= nx - HALO)
    for z in range(cz):
        for v in range(VARS):
            patch = pltpu.roll(merged[v], (nx - HALO - 2 - GROUP * z) % nx, 1)
            rows = cell_rows(v, z)
            total[rows, :] = total[rows, :] + jnp.where(rim, patch, 0.0)
            kept[rows, :] = base[v, z] * (1.0 / 3.0) + (2.0 / 3.0) * now[v, z]

    if direct:
        pl.when(lowest)(send_down_around)
    down.wait_recv()
    high_edge()

    def set_scale(top):
        step = (2.0 / 3.0 * 0.3) / jnp.max(top, keepdims=True)
        scale[...] = jnp.broadcast_to(step, (ny, nx))

    low_edge(range(HALO - 1, 0, -1), (0, 1), (4, 5))

    if direct:

        @pl.when(early)
        def _():
            arrivals(top_first, size - 1, first_in)
            top = top_first[0]
            for d in range(1, size):
                top = jnp.maximum(top, top_first[d])
            mine[1] = top

            @pl.when(caster)
            def _():
                for copy in cast:
                    copy.start()

            set_scale(top)

    down.wait_send()
    for copy in up:
        copy.wait_send()
    pl.when(outer)(to_high.wait_send)
    pl.when(inner)(to_low.wait_send)
    if direct:
        for h in range(HUBS):
            pl.when(jnp.logical_not(hubs[h]))(to_hub[h].wait_send)
    else:
        arrivals(top_first, len(across), first_out)
        arrivals(top_second, len(along), second_out)

    low_edge([0], (4, 5), None)

    if direct:

        @pl.when(caster)
        def _():
            arrivals(top_first, len(cast), second_out)

        @pl.when(jnp.logical_not(early))
        def _():
            cast[0].wait_recv()
            set_scale(mine[2])

    else:
        arrivals(top_second, len(along), second_in)
        top = mine[1]
        for d in range(len(along)):
            top = jnp.maximum(top, top_second[d])
        set_scale(top)


def finish(ny, kept, total, scale, out_ref):
    step = scale[...]
    for i in range(kept.shape[0] // ny):
        rows = pl.ds(i * ny, ny)
        out_ref[rows, :] = kept[rows, :] + step * total[rows, :]


def solution(mesh):
    n_stream, n_cross = mesh.shape["stream"], mesh.shape["cross"]
    direct = n_stream * n_cross <= DIRECT
    first = n_stream * n_cross if direct else n_cross - 1

    def shards(state_now, state_base, inflow):
        _, cz, ny, nx = state_now.shape
        f32 = jnp.float32
        vmem = lambda *shape: pltpu.VMEM(shape, f32)
        dma = lambda n: pltpu.SemaphoreType.DMA((n,))
        cells = VARS * cz * ny
        kept, total, scale = pl.pallas_call(
            functools.partial(kernel, (n_stream, n_cross, cz, ny, nx), direct),
            out_shape=(
                vmem(cells, nx),
                vmem(cells, nx),
                vmem(ny, nx),
            ),
            in_specs=[pl.BlockSpec(memory_space=pl.ANY)] * 3,
            out_specs=[pl.BlockSpec(memory_space=pltpu.VMEM)] * 3,
            scratch_shapes=[
                vmem(*state_now.shape),
                vmem(*state_now.shape),
                vmem(VARS, HALO, cz, ny),
                vmem(HALO, cz, nx),
                vmem(nx, nx),
                vmem((cz + 2 * HALO) * VARS * ny, nx),
                vmem((ny + 2 * HALO) * VARS * cz, nx),
                vmem(4, VARS, ny, nx),
                vmem(3, VARS, ny, nx),
                vmem(2, VARS + 1, ny, nx),
                vmem(VARS * ny, nx),
                vmem(VARS * ny, nx),
                vmem(VARS * ny, nx),
                vmem(6, VARS + 1, cz, nx),
                vmem(first, 1, nx),
                vmem(n_stream - 1, 1, nx),
                vmem(3, 1, nx),
                dma(3),
                dma(3 + HALO),
                dma(3 + HALO),
                dma(HUBS),
                dma(1),
                dma(1),
                dma(1),
                pltpu.SemaphoreType.REGULAR((3,)),
            ],
            compiler_params=pltpu.CompilerParams(collective_id=0, has_side_effects=True),
        )(state_now, state_base, jnp.transpose(inflow, (0, 3, 1, 2)))
        kept, total, scale = [
            pltpu.with_memory_space_constraint(x, pltpu.VMEM) for x in (kept, total, scale)
        ]
        out = pl.pallas_call(
            functools.partial(finish, ny),
            out_shape=jax.ShapeDtypeStruct((cells, nx), f32),
            in_specs=[pl.BlockSpec(memory_space=pltpu.VMEM)] * 3,
            out_specs=pl.BlockSpec(memory_space=pltpu.VMEM),
        )(kept, total, scale)
        return out.reshape(state_now.shape)

    split = P(None, None, "cross", "stream")
    return jax.shard_map(
        shards,
        mesh=mesh,
        in_specs=(split, split, P(None, None, "cross", None)),
        out_specs=split,
        check_vma=False,
    )
```

```python
import functools

import jax
import jax.numpy as jnp
from jax import lax
from jax.experimental import pallas as pl
from jax.experimental.pallas import tpu as pltpu
from jax.sharding import PartitionSpec as P

MESH = pl.DeviceIdType.MESH
VARS = 7
HALO = 3
GROUP = 8
DIRECT = 64
HUBS = 2
STIFF = 4.4 * 0.6 / 3.4


def recip(x):
    return 1.0 / x


def mixture(volume):
    rest = 1.0 - volume
    return volume * (1.0 / 0.4) + rest * (1.0 / 3.4), rest * STIFF


def primitive(u):
    inv = recip(u[0] + u[1])
    vx, vy, vz = u[2] * inv, u[3] * inv, u[4] * inv
    gam, stiff = mixture(u[6])
    kinetic = 0.5 * (u[2] * vx + u[3] * vy + u[4] * vz)
    return [u[0], u[1], vx, vy, vz, (u[5] - kinetic - stiff) * recip(gam), u[6]]


def max_speed(w):
    gam, stiff = mixture(w[6])
    top = (gam + 1.0) * w[5] + stiff
    sound = jnp.sqrt(top * recip(gam * (w[0] + w[1])))
    return jnp.maximum(jnp.maximum(jnp.abs(w[2]), jnp.abs(w[3])), jnp.abs(w[4])) + sound


def weno_pair(f, g, h, k, l):
    e1, e2, e3, e4 = g - f, h - g, k - h, l - k
    s0, s1, s2 = e2 - e1, e3 - e2, e4 - e3
    d2, d3 = e2 + e2, e3 + e3
    t0, t1, t2 = d2 + s0, e2 + e3, d3 - s2
    eps = 1e-6 * 12.0 / 13.0
    r0 = recip(s0 * s0 + (eps + (3.0 / 13.0) * (t0 * t0)))
    r1 = recip(s1 * s1 + (eps + (3.0 / 13.0) * (t1 * t1)))
    r2 = recip(s2 * s2 + (eps + (3.0 / 13.0) * (t2 * t2)))
    a0, a1, a2 = r0 * r0, 6.0 * (r1 * r1), r2 * r2
    b0, b2 = 3.0 * a0, 3.0 * a2
    p0, p2 = t0 + e2, t2 + e3
    up = (a0 * (p0 + s0) + a1 * (d3 + e2) + b2 * p2) * recip(6.0 * (a0 + a1 + b2))
    down = (a2 * (p2 - s2) + a1 * (d2 + e3) + b0 * p0) * recip(6.0 * (a2 + a1 + b0))
    return h + up, h - down


def limit(state, low, high):
    out = list(state)
    for v in (0, 1, 5):
        out[v] = jnp.maximum(state[v], low[v])
    out[6] = jnp.minimum(jnp.maximum(state[6], low[6]), high)
    return out


def side(w, normal):
    dens = w[0] + w[1]
    gam, stiff = mixture(w[6])
    m = [dens * w[2], dens * w[3], dens * w[4]]
    heat = gam * w[5] + stiff
    energy = heat + 0.5 * (m[0] * w[2] + m[1] * w[3] + m[2] * w[4])
    vn = w[2 + normal]
    amounts = [w[0], w[1], m[0], m[1], m[2], energy, w[6]]
    moved = [q * vn for q in amounts]
    moved[2 + normal] = moved[2 + normal] + w[5]
    moved[5] = (energy + w[5]) * vn
    sound = jnp.sqrt((heat + w[5]) * recip(gam * dens))
    return amounts, moved, vn, jnp.abs(vn) + sound


def faces(left, right, below, above, normal):
    low = {v: 0.5 * jnp.minimum(below[v], above[v]) for v in (0, 1, 5, 6)}
    high = 1.0 - 0.5 * (1.0 - jnp.maximum(below[6], above[6]))
    ul, fl, nl, sl = side(limit(left, low, high), normal)
    ur, fr, nr, sr = side(limit(right, low, high), normal)
    fast = 0.5 * jnp.maximum(sl, sr)
    out = [0.5 * (fl[v] + fr[v]) - fast * (ur[v] - ul[v]) for v in range(VARS)]
    return out + [0.5 * (nl + nr)]


def rate(lo, hi, volume):
    out = [lo[v] - hi[v] for v in range(VARS)]
    out[6] = out[6] + volume * (hi[7] - lo[7])
    return out


def reader(src, height):
    def at(c, v):
        return src[pl.ds(pl.multiple_of((c * VARS + v) * height, height), height), :]

    def row(c):
        return [at(c, v) for v in range(VARS)]

    def states(c):
        pairs = [weno_pair(*[at(c + o, v) for o in range(-2, 3)]) for v in range(VARS)]
        return [p[0] for p in pairs], [p[1] for p in pairs]

    return at, row, states


def sweep(src, count, height, normal, emit):
    at, row, states = reader(src, height)

    def cell(c, left):
        after, right = states(c)
        return faces(left, right, row(c - 1), row(c), normal), after

    flux, left = cell(HALO, states(HALO - 1)[0])

    def step(i, carry):
        left, lo = carry
        hi, left = cell(i + HALO + 1, left)
        emit(i, rate(lo, hi, at(i + HALO, 6)))
        return left, hi

    lax.fori_loop(0, count, step, (left, flux))


def kernel(
    dims,
    direct,
    now_hbm,
    base_hbm,
    inflow_hbm,
    kept,
    total,
    scale,
    now,
    base,
    inflow,
    flat,
    wide,
    wz,
    wy,
    shifted,
    sided,
    fluxes,
    pack,
    from_low,
    from_high,
    joint,
    top_first,
    top_second,
    mine,
    load_sem,
    halo_send,
    halo_recv,
    first_send,
    first_recv,
    second_send,
    second_recv,
    ready_sem,
):
    n_stream, n_cross, cz, ny, nx = dims
    tile = VARS * ny
    ztile = VARS * cz
    half = cz * GROUP
    ms, mc = lax.axis_index("stream"), lax.axis_index("cross")

    loads = [
        pltpu.make_async_copy(base_hbm, base, load_sem.at[0]),
        pltpu.make_async_copy(now_hbm, now, load_sem.at[1]),
        pltpu.make_async_copy(inflow_hbm, inflow, load_sem.at[2]),
    ]
    highest = mc == n_cross - 1
    urgent = highest & (ms < HUBS)

    def load_now():
        for v in range(VARS):
            pltpu.make_async_copy(now_hbm.at[v], now.at[v], load_sem.at[1]).start()

    if direct:
        pl.when(urgent)(load_now)
    for v in range(VARS):
        pltpu.make_async_copy(base_hbm.at[v], base.at[v], load_sem.at[0]).start()
    if direct:
        pl.when(jnp.logical_not(urgent))(load_now)
    else:
        load_now()
    loads[2].start()

    size = n_stream * n_cross
    across = [(0, d) for d in range(1, n_cross)]
    along = [(d, 0) for d in range(1, n_stream)]
    others = [(d, e) for e in range(n_cross) for d in range(n_stream) if (d, e) != (0, 0)]
    inner, outer = ms > 0, ms < n_stream - 1
    lowest = mc == 0
    hubs = [(ms == h) & lowest for h in range(HUBS)]
    early = functools.reduce(jnp.logical_or, hubs)
    caster = hubs[HUBS - 1]

    def device(offset):
        return {
            "stream": lax.rem(ms + offset[0], n_stream),
            "cross": lax.rem(mc + offset[1], n_cross),
        }

    barrier = pltpu.get_barrier_semaphore()

    def greet(target):
        pl.semaphore_signal(barrier, device_id=target, device_id_type=MESH)

    above, below = device((0, 1)), device((0, n_cross - 1))
    after, before = device((1, 0)), device((n_stream - 1, 0))

    def ready(k, target):
        pl.semaphore_signal(ready_sem.at[k], device_id=target, device_id_type=MESH)

    def await_ready(k):
        pl.semaphore_wait(ready_sem.at[k], 1)

    if direct:
        pl.when(jnp.logical_not(highest))(lambda: greet(above))
        pl.when(lowest)(lambda: greet(below))
        pl.when(outer)(lambda: greet(after))

        @pl.when(early)
        def _():
            for p in others:
                greet(device(p))

        one = lambda flag: jnp.where(flag, 1, 0)
        greetings = jnp.where(early, HUBS - 1, HUBS)
        pl.semaphore_wait(
            barrier, greetings + one(inner) + one(highest) + one(jnp.logical_not(lowest))
        )
        pl.when(highest)(lambda: ready(2, above))
        pl.when(jnp.logical_not(lowest))(lambda: ready(0, below))
        pl.when(inner)(lambda: ready(1, before))
    else:
        for p in across + along:
            greet(device(p))
        pl.semaphore_wait(barrier, n_cross + n_stream - 2)

    def remote(src, dst, send, recv, target):
        return pltpu.make_async_remote_copy(
            src_ref=src,
            dst_ref=dst,
            send_sem=send,
            recv_sem=recv,
            device_id=target,
            device_id_type=MESH,
        )

    def spread(slot, buffer, offsets, send, recv):
        return [
            remote(mine.at[slot], buffer.at[i], send, recv, device(p))
            for i, p in enumerate(offsets)
        ]

    def arrivals(buffer, count, recv):
        part = buffer.at[pl.ds(0, count)]
        pltpu.make_async_copy(part, part, recv).wait()

    first_out, first_in = first_send.at[0], first_recv.at[0]
    second_out, second_in = second_send.at[0], second_recv.at[0]
    if direct:
        spot_here = ms * n_cross + mc
        to_hub = [
            remote(
                mine.at[0],
                top_first.at[spot_here],
                first_send.at[h],
                first_in,
                {"stream": h, "cross": 0},
            )
            for h in range(HUBS)
        ]
        cast = [
            remote(mine.at[1], mine.at[2], second_out, second_in, {"stream": d, "cross": e})
            for e in range(n_cross)
            for d in range(n_stream)
            if e > 0 or d >= HUBS
        ]
    else:
        first = spread(0, top_first, across, first_out, first_in)
        second = spread(1, top_second, along, second_out, second_in)

    def send_speed():
        if direct:
            for h in range(HUBS):
                pl.when(jnp.logical_not(hubs[h]))(to_hub[h].start)
        else:
            for copy in first:
                copy.start()

    rows = HALO * ztile
    down = remote(
        wy.at[pl.ds(rows, rows)],
        wy.at[pl.ds((HALO + ny) * ztile, rows)],
        halo_send.at[0],
        halo_recv.at[0],
        below,
    )
    up = [
        remote(
            wy.at[pl.ds((ny + k) * ztile, ztile)],
            wy.at[pl.ds(k * ztile, ztile)],
            halo_send.at[3 + k],
            halo_recv.at[3 + k],
            above,
        )
        for k in range(HALO)
    ]
    to_high = pltpu.make_async_remote_copy(
        src_ref=pack,
        dst_ref=from_low,
        send_sem=halo_send.at[1],
        recv_sem=halo_recv.at[1],
        device_id=after,
        device_id_type=MESH,
    )
    to_low = pltpu.make_async_remote_copy(
        src_ref=pack,
        dst_ref=from_high,
        send_sem=halo_send.at[2],
        recv_sem=halo_recv.at[2],
        device_id=before,
        device_id_type=MESH,
    )

    def send_up():
        for copy in reversed(up):
            copy.start()

    def send_up_ready():
        await_ready(0)
        send_up()

    def send_down():
        down.start()

    def send_down_around():
        await_ready(2)
        down.start()

    def send_after():
        if direct:
            await_ready(1)
        to_high.start()

    def by_plane(y):
        for v in range(VARS):
            wy[pl.ds((HALO + y) * ztile + v * cz, cz), :] = wz[
                pl.ds(HALO * tile + v * ny + y, cz, stride=tile), :
            ]

    def measure_speed():
        loads[0].wait()
        speed = None
        for z in range(cz):
            s = max_speed(primitive([base[v, z] for v in range(VARS)]))
            speed = s if speed is None else jnp.maximum(speed, s)
        mine[0] = jnp.max(speed, axis=0, keepdims=True)
        if direct:
            top_first[spot_here] = mine[0]
        send_speed()


    if direct:
        pl.when(jnp.logical_not(urgent))(measure_speed)
    else:
        measure_speed()

    loads[1].wait()
    lane = lax.broadcasted_iota(jnp.int32, (ny, nx), 1)
    group = lane // GROUP
    for z in range(cz):
        w = primitive([now[v, z] for v in range(VARS)])
        spots = [HALO + z]
        if z < HALO:
            spots.append(HALO + cz + z)
        if z >= cz - HALO:
            spots.append(z - (cz - HALO))
        for v in range(VARS):
            for c in spots:
                wz[pl.ds(c * tile + v * ny, ny), :] = w[v]
    for y in range(ny):
        by_plane(y)
    if direct:

        @pl.when(urgent)
        def _():
            up[HALO - 1].start()
            measure_speed()
            for copy in reversed(up[: HALO - 1]):
                copy.start()

        pl.when(jnp.logical_not(highest | lowest))(send_down)
    else:
        send_up()
        send_down()

    for v in range(VARS):
        packed = None
        for z in range(cz):
            w = wz[pl.ds((HALO + z) * tile + v * ny, ny), :]
            upper = pltpu.roll(w, (GROUP * z - (nx - 5)) % nx, 1)
            lower = pltpu.roll(w, (half + GROUP * z + HALO) % nx, 1)
            piece = jnp.where(group == z, upper, lower)
            if z == 0:
                packed = piece
            else:
                packed = jnp.where((group == z) | (group == cz + z), piece, packed)
        pack[pl.ds(v * ny, ny), :] = packed
    pl.when(inner)(to_low.start)
    if direct:
        pl.when(highest & ((ms >= HUBS)))(send_up)

    def stream_shifts(w):
        return [[pltpu.roll(x, d % nx, 1) for x in w] for d in (2, 1, -1, -2)]

    def stream_states(shifts, w):
        m2, m1, p1, p2 = shifts
        pairs = [weno_pair(m2[v], m1[v], w[v], p1[v], p2[v]) for v in range(VARS)]
        return [pltpu.roll(p[0], 1, 1) for p in pairs], [p[1] for p in pairs]

    def ahead(lo):
        return [pltpu.roll(f, nx - 1, 1) for f in lo]

    def cell_rows(v, z):
        return pl.ds(pl.multiple_of((v * cz + z) * ny, ny), ny)

    def keep_rate(z, out):
        for v in range(VARS):
            total[cell_rows(v, z), :] = out[v]

    sweep(wz, cz, ny, 2, keep_rate)

    pl.when(outer)(send_after)
    if direct:
        pl.when(jnp.logical_not(highest))(send_up_ready)

    whole = (lane >= HALO) & (lane < nx - 2)

    def centre(z):
        return [
            wz[pl.ds(pl.multiple_of(((HALO + z) * VARS + v) * ny, ny), ny), :]
            for v in range(VARS)
        ]

    def stage_shift(z):
        for d, row in enumerate(stream_shifts(centre(z))):
            for v in range(VARS):
                shifted[d, v] = row[v]

    def stage_state(z):
        shifts = [[shifted[d, v] for v in range(VARS)] for d in range(4)]
        left, right = stream_states(shifts, centre(z))
        for v in range(VARS):
            sided[0, v] = left[v]
            sided[1, v] = right[v]
            sided[2, v] = shifts[1][v]

    def stage_flux(z):
        left, right, below = [[sided[k, v] for v in range(VARS)] for k in range(3)]
        lo = [jnp.where(whole, f, 0.0) for f in faces(left, right, below, centre(z), 0)]
        hi = ahead(lo)
        for o in range(VARS + 1):
            fluxes[0, o] = lo[o]
            fluxes[1, o] = hi[o]

    def stage_rate(z):
        lo, hi = [[fluxes[k, o] for o in range(VARS + 1)] for k in range(2)]
        out = rate(lo, hi, centre(z)[6])
        for v in range(VARS):
            total[cell_rows(v, z), :] = total[cell_rows(v, z), :] + out[v]

    stages = (stage_shift, stage_state, stage_flux, stage_rate)
    depth = len(stages)

    def advance(z):
        for k in reversed(range(depth)):
            stages[k](z - k)

    for z in range(depth - 1):
        for k in reversed(range(z + 1)):
            stages[k](z - k)
    lax.fori_loop(depth - 1, cz, lambda z, c: (advance(z), c)[1], 0)
    for z in range(cz, cz + depth - 1):
        for k in reversed(range(z - cz + 1, depth)):
            stages[k](z - k)

    if direct:
        pl.when(highest)(send_down)

    def add_rate(y, out):
        for v in range(VARS):
            rows = pl.ds(v * cz * ny + y, cz, stride=ny)
            total[rows, :] = total[rows, :] + out[v]

    wy_at, wy_row, wy_states = reader(wy, cz)

    def cross_face(y, left, right):
        return faces(left, right, wy_row(HALO + y - 1), wy_row(HALO + y), 1)

    def cross_rate(y, lo, hi):
        add_rate(y, rate(lo, hi, wy_at(HALO + y, 6)))

    def save(slot, values):
        for k, x in enumerate(values):
            joint[slot, k] = x

    def saved(slot, size):
        return [joint[slot, k] for k in range(size)]

    left, right = wy_states(2 * HALO - 1)
    save(0, right)
    lo = None
    for y in range(HALO, ny - HALO + 1):
        after, right = wy_states(HALO + y)
        hi = cross_face(y, left, right)
        if lo is None:
            save(1, hi)
        else:
            cross_rate(y - 1, lo, hi)
        left, lo = after, hi
    save(2, left)
    save(3, lo)

    def low_edge(cells, joint_in, joint_out):
        ahead_flux, next_right = saved(joint_in[1], VARS + 1), saved(joint_in[0], VARS)
        for y in cells:
            up[y].wait_recv()
            left, right = wy_states(HALO + y - 1)
            lo = cross_face(y, left, next_right)
            cross_rate(y, lo, ahead_flux)
            ahead_flux, next_right = lo, right
        if joint_out:
            save(joint_out[0], next_right)
            save(joint_out[1], ahead_flux)

    def high_edge():
        left, lo = saved(2, VARS), saved(3, VARS + 1)
        for y in range(ny - HALO + 1, ny + 1):
            after, right = wy_states(HALO + y)
            hi = cross_face(y, left, right)
            cross_rate(y - 1, lo, hi)
            left, lo = after, hi

    if not direct:
        arrivals(top_first, len(across), first_in)
        slab = mine[0]
        for d in range(len(across)):
            slab = jnp.maximum(slab, top_first[d])
        mine[1] = slab
        for copy in second:
            copy.start()

    loads[2].wait()

    @pl.when(ms == 0)
    def _():
        for k in range(HALO):
            for v in range(VARS):
                flat[k, :, pl.ds(v * ny, ny)] = inflow[v, k]
            wide[pl.ds(half + k, cz, stride=GROUP), :] = flat[k]
        turned = jnp.transpose(wide[...])
        w = primitive([turned[v * ny : (v + 1) * ny] for v in range(VARS)])
        for v in range(VARS):
            from_low[pl.ds(v * ny, ny), :] = w[v]

    @pl.when(ms > 0)
    def _():
        to_high.wait_recv()

    spot = lane % GROUP

    @pl.when(ms == n_stream - 1)
    def _():
        for v in range(VARS):
            own = pack[pl.ds(v * ny, ny), :]
            copies = [pltpu.roll(own, k, 1) for k in (1, 2, 3)]
            from_high[pl.ds(v * ny, ny), :] = jnp.where(
                spot == 5, copies[0], jnp.where(spot == 6, copies[1], copies[2])
            )

    @pl.when(ms < n_stream - 1)
    def _():
        to_low.wait_recv()

    upper_side = lane < half
    edge = []
    for v in range(VARS):
        own = pack[pl.ds(v * ny, ny), :]
        low, high = from_low[pl.ds(v * ny, ny), :], from_high[pl.ds(v * ny, ny), :]
        edge.append(
            jnp.where(
                upper_side,
                jnp.where(spot < 5, own, high),
                jnp.where(spot < HALO, low, own),
            )
        )
    shifts = stream_shifts(edge)
    edge_left, edge_right = stream_states(shifts, edge)
    edge_faces = faces(edge_left, edge_right, shifts[1], edge, 0)
    middle = (spot >= HALO) & (spot < 2 * HALO)
    lo = [jnp.where(middle, f, 0.0) for f in edge_faces]
    hi = ahead(lo)
    merged = []
    for out in rate(lo, hi, edge[6]):
        upper = jnp.where(upper_side & (spot >= 2) & (spot < 5), out, 0.0)
        lower = jnp.where(jnp.logical_not(upper_side) & middle, out, 0.0)
        merged.append(upper + pltpu.roll(lower, nx - half + 2, 1))
    rim = (lane < HALO) | (lane >= nx - HALO)
    for z in range(cz):
        for v in range(VARS):
            patch = pltpu.roll(merged[v], (nx - HALO - 2 - GROUP * z) % nx, 1)
            rows = cell_rows(v, z)
            total[rows, :] = total[rows, :] + jnp.where(rim, patch, 0.0)
            kept[rows, :] = base[v, z] * (1.0 / 3.0) + (2.0 / 3.0) * now[v, z]

    if direct:
        pl.when(lowest)(send_down_around)
    down.wait_recv()
    high_edge()

    def set_scale(top):
        step = (2.0 / 3.0 * 0.3) / jnp.max(top, keepdims=True)
        scale[...] = jnp.broadcast_to(step, (ny, nx))

    low_edge(range(HALO - 1, 0, -1), (0, 1), (4, 5))

    if direct:

        @pl.when(early)
        def _():
            arrivals(top_first, size - 1, first_in)
            top = top_first[0]
            for d in range(1, size):
                top = jnp.maximum(top, top_first[d])
            mine[1] = top

            @pl.when(caster)
            def _():
                for copy in cast:
                    copy.start()

            set_scale(top)

    down.wait_send()
    for copy in up:
        copy.wait_send()
    pl.when(outer)(to_high.wait_send)
    pl.when(inner)(to_low.wait_send)
    if direct:
        for h in range(HUBS):
            pl.when(jnp.logical_not(hubs[h]))(to_hub[h].wait_send)
    else:
        arrivals(top_first, len(across), first_out)
        arrivals(top_second, len(along), second_out)

    low_edge([0], (4, 5), None)

    if direct:

        @pl.when(caster)
        def _():
            arrivals(top_first, len(cast), second_out)

        @pl.when(jnp.logical_not(early))
        def _():
            cast[0].wait_recv()
            set_scale(mine[2])

    else:
        arrivals(top_second, len(along), second_in)
        top = mine[1]
        for d in range(len(along)):
            top = jnp.maximum(top, top_second[d])
        set_scale(top)


def finish(ny, kept, total, scale, out_ref):
    step = scale[...]
    for i in range(kept.shape[0] // ny):
        rows = pl.ds(i * ny, ny)
        out_ref[rows, :] = kept[rows, :] + step * total[rows, :]


def solution(mesh):
    n_stream, n_cross = mesh.shape["stream"], mesh.shape["cross"]
    direct = n_stream * n_cross <= DIRECT
    first = n_stream * n_cross if direct else n_cross - 1

    def shards(state_now, state_base, inflow):
        _, cz, ny, nx = state_now.shape
        f32 = jnp.float32
        vmem = lambda *shape: pltpu.VMEM(shape, f32)
        dma = lambda n: pltpu.SemaphoreType.DMA((n,))
        cells = VARS * cz * ny
        kept, total, scale = pl.pallas_call(
            functools.partial(kernel, (n_stream, n_cross, cz, ny, nx), direct),
            out_shape=(
                vmem(cells, nx),
                vmem(cells, nx),
                vmem(ny, nx),
            ),
            in_specs=[pl.BlockSpec(memory_space=pl.ANY)] * 3,
            out_specs=[pl.BlockSpec(memory_space=pltpu.VMEM)] * 3,
            scratch_shapes=[
                vmem(*state_now.shape),
                vmem(*state_now.shape),
                vmem(VARS, HALO, cz, ny),
                vmem(HALO, cz, nx),
                vmem(nx, nx),
                vmem((cz + 2 * HALO) * VARS * ny, nx),
                vmem((ny + 2 * HALO) * VARS * cz, nx),
                vmem(4, VARS, ny, nx),
                vmem(3, VARS, ny, nx),
                vmem(2, VARS + 1, ny, nx),
                vmem(VARS * ny, nx),
                vmem(VARS * ny, nx),
                vmem(VARS * ny, nx),
                vmem(6, VARS + 1, cz, nx),
                vmem(first, 1, nx),
                vmem(n_stream - 1, 1, nx),
                vmem(3, 1, nx),
                dma(3),
                dma(3 + HALO),
                dma(3 + HALO),
                dma(HUBS),
                dma(1),
                dma(1),
                dma(1),
                pltpu.SemaphoreType.REGULAR((3,)),
            ],
            compiler_params=pltpu.CompilerParams(collective_id=0, has_side_effects=True),
        )(state_now, state_base, jnp.transpose(inflow, (0, 3, 1, 2)))
        kept, total, scale = [
            pltpu.with_memory_space_constraint(x, pltpu.VMEM) for x in (kept, total, scale)
        ]
        out = pl.pallas_call(
            functools.partial(finish, ny),
            out_shape=jax.ShapeDtypeStruct((cells, nx), f32),
            in_specs=[pl.BlockSpec(memory_space=pltpu.VMEM)] * 3,
            out_specs=pl.BlockSpec(memory_space=pltpu.VMEM),
        )(kept, total, scale)
        return out.reshape(state_now.shape)

    split = P(None, None, "cross", "stream")
    return jax.shard_map(
        shards,
        mesh=mesh,
        in_specs=(split, split, P(None, None, "cross", None)),
        out_specs=split,
        check_vma=False,
    )
```
